128 devices in a mesh: row: 32 (over x, z, core), col: 4 (over y).
Axes of the slice: x: 4, y: 4, z: 4, core: 2. Of those that a mesh axis runs over, the one named last changes fastest.
Arguments:
- graph_one: bfloat16 [16384, 16384], P('row'), may hold values from -64 to 64
- graph_two: bfloat16 [2048, 2048], P('col'), may hold values from -64 to 64
- coupling: float32 [16384, 2048], P('row', 'col'), may hold values from 0.2 to 5
- sizes_one: int32 [32], replicated, may hold values from 256 to 512
- sizes_two: int32 [4], replicated, may hold values from 256 to 512
Outputs:
- new_coupling: float32 [16384, 2048], P('row', 'col')
- row_potential: float32 [16384], P('row')
- col_potential: float32 [2048], P('col')
The draws below stay inside these ranges and needn't reach their ends.
All inputs are finite; a program needn't handle non-finite values.
Results may differ from the reference program's by a relative error of at most 0.007.
The reference program's roundings to bfloat16 on the way (of `rounded_plan` and `first_product`) count: a program that leaves them out, or rounds other values in their place, can miss the bound.
Values may be sent and summed in bfloat16 or wider, within the bound.
A program may use at most 128 MiB of HBM per device.

```python
import math
import jax
import jax.numpy as jnp
from jax import lax

BLOCK = 512
SWEEPS = 5
N1 = 16384
N2 = 2048
NB1 = 32
NB2 = 4


def symmetric_draw(key, count):
    raw = jnp.clip(jax.random.normal(jax.random.fold_in(key, 11), (count, count), jnp.float32), -5.0, 5.0)
    matrix = (raw + raw.T) * 0.5 ** 0.5
    return matrix.astype(jnp.bfloat16)


def draw_graph_one(key, part):
    return symmetric_draw(jax.random.fold_in(key, 21), N1)


def draw_graph_two(key, part):
    return symmetric_draw(jax.random.fold_in(key, 22), N2)


def with_ends(drawn, key, smallest, largest):
    extent = drawn.shape
    index_at = [jax.random.randint(jax.random.fold_in(key, axis), (), 0, extent[axis]) for axis in range(len(extent))]
    drawn = drawn.at[tuple(index_at)].set(smallest)
    longest = extent.index(max(extent))
    index_at[longest] = (index_at[longest] + 1) % extent[longest]
    return drawn.at[tuple(index_at)].set(largest)


def shard_levels(stream_key, shape, shards, least, top_value):
    gain = 1.0
    for position, blocks in shards:
        heights = jax.random.uniform(jax.random.fold_in(jax.random.fold_in(stream_key, 6), position), (blocks,), jnp.float32, least / len(shards), top_value / len(shards))
        gain = gain * jnp.repeat(jnp.exp(heights), shape[position] // blocks).reshape((-1,) + (1,) * (len(shape) - 1 - position))
    return gain


def setup_inputs(seed: int = 0) -> dict:
    streams_of = jax.random.split(jax.random.key(seed), 6)
    return {
        "graph_one": draw_graph_one(jax.random.fold_in(streams_of[5], 71), 0),
        "graph_two": draw_graph_two(jax.random.fold_in(streams_of[5], 71), 0),
        "coupling": jnp.clip(jnp.exp(math.log(5.0) - 3.218876 * jax.random.uniform(streams_of[2], (N1, N2), jnp.float32) ** shard_levels(streams_of[2], (N1, N2), ((0, 32), (1, 4)), -0.2, 0.2)), 0.2, 5.0),
        "sizes_one": with_ends(jax.random.randint(streams_of[3], (NB1,), BLOCK // 2, BLOCK + 1), jax.random.fold_in(streams_of[3], 1), BLOCK // 2, BLOCK).astype(jnp.int32),
        "sizes_two": with_ends(jax.random.randint(streams_of[4], (NB2,), BLOCK // 2, BLOCK + 1), jax.random.fold_in(streams_of[4], 1), BLOCK // 2, BLOCK).astype(jnp.int32),
    }


def reference(graph_one, graph_two, coupling, sizes_one, sizes_two):
    count_one = graph_one.shape[0]
    count_two = graph_two.shape[0]
    live_one = (jnp.arange(count_one, dtype=jnp.int32) % BLOCK < jnp.repeat(sizes_one, BLOCK, total_repeat_length=count_one)).astype(jnp.int32)
    live_two = (jnp.arange(count_two, dtype=jnp.int32) % BLOCK < jnp.repeat(sizes_two, BLOCK, total_repeat_length=count_two)).astype(jnp.int32)
    total_one = jnp.sum(sizes_one).astype(jnp.float32)
    total_two = jnp.sum(sizes_two).astype(jnp.float32)
    mask_one = live_one > 0
    mask_two = live_two > 0
    live_both = mask_one[:, None] & mask_two[None, :]
    rounded_plan = jnp.where(live_both, coupling, jnp.float32(0.0)).astype(jnp.bfloat16)
    first_product = jnp.dot(graph_one, rounded_plan, preferred_element_type=jnp.float32).astype(jnp.bfloat16)
    cross_term = jnp.dot(first_product, graph_two, preferred_element_type=jnp.float32)
    row_const = lax.optimization_barrier(jnp.sum(jnp.square(graph_one.astype(jnp.float32)) * live_one.astype(jnp.float32)[None, :], axis=1)) / total_one
    col_const = lax.optimization_barrier(jnp.sum(jnp.square(graph_two.astype(jnp.float32)) * live_two.astype(jnp.float32)[None, :], axis=1)) / total_two
    mass_scale = float(count_one * count_two)
    epsilon = 1.0 / math.sqrt(mass_scale)
    reduced_cost = -2.0 / mass_scale * cross_term
    reduced_col = jnp.zeros((count_two,), jnp.float32)
    reduced_row = jnp.zeros((count_one,), jnp.float32)
    for sweep_index in range(SWEEPS):
        row_values = (reduced_col[None, :] - reduced_cost) / epsilon
        row_lse = jax.nn.logsumexp(jnp.where(mask_two[None, :], row_values, -jnp.inf), axis=1)
        reduced_row = jnp.where(mask_one, -epsilon * jnp.log(total_one) - epsilon * row_lse, jnp.float32(0.0))
        col_values = (reduced_row[:, None] - reduced_cost) / epsilon
        col_lse = jax.nn.logsumexp(jnp.where(mask_one[:, None], col_values, -jnp.inf), axis=0)
        reduced_col = jnp.where(mask_two, -epsilon * jnp.log(total_two) - epsilon * col_lse, jnp.float32(0.0))
    exponent = (reduced_row[:, None] + reduced_col[None, :] - reduced_cost) / epsilon
    new_coupling = jnp.where(live_both, mass_scale * jnp.exp(exponent), jnp.float32(0.0))
    row_potential = jnp.where(mask_one, reduced_row + row_const, jnp.float32(0.0))
    col_potential = jnp.where(mask_two, reduced_col + col_const, jnp.float32(0.0))
    return (new_coupling, row_potential, col_potential)
```

```python
import functools
import math

import jax
import jax.numpy as jnp
from jax import lax
from jax.experimental import pallas as pl
from jax.experimental.pallas import tpu as pltpu
from jax.sharding import PartitionSpec as P

BLOCK = 512
SWEEPS = 5
LANES = 128
TILES = BLOCK // LANES
CHUNK = 64
MESH = pl.DeviceIdType.MESH

very_low = -1e30


def copy_for_each(shard, axis):
    copies = jnp.broadcast_to(shard, (lax.axis_size(axis), *shard.shape))
    return lax.all_to_all(copies, axis, split_axis=0, concat_axis=0, tiled=True)


def in_order(blocks, dim):
    blocks = jnp.moveaxis(blocks, 0, dim)
    lengths = blocks.shape
    return blocks.reshape(*lengths[:dim], lengths[dim] * lengths[dim + 1], *lengths[dim + 2 :])


def gather_directly(shard, axis, dim):
    return in_order(copy_for_each(shard, axis), dim)


def live_slots(sizes, count):
    return (
        jnp.arange(BLOCK, dtype=jnp.int32)[None, :] < sizes[:, None]
    ).reshape(count)


def plane_neighbours():
    steps = []
    for dx in range(4):
        for dz in range(4):
            for dc in range(2):
                if dx or dz or dc:
                    far = min(dx, 4 - dx) + min(dz, 4 - dz)
                    steps.append((-far, -dc, dx, dz, dc))
    return [step[2:] for step in sorted(steps)]


def row_index(x, z, core):
    return (x * 4 + z) * 2 + core


def diagonal():
    return lax.broadcasted_iota(jnp.int32, (LANES, LANES), 0) == lax.broadcasted_iota(
        jnp.int32, (LANES, LANES), 1
    )


def sinkhorn_kernel(
    mass_scale,
    cross_ref,
    row_const_ref,
    col_const_ref,
    sizes_one_ref,
    sizes_two_ref,
    plan_ref,
    row_ref,
    col_ref,
    cost_ref,
    rho_ref,
    row_box,
    col_box,
    row_send,
    row_recv,
    col_send,
    col_recv,
):
    row = lax.axis_index("row")
    col = lax.axis_index("col")
    x, z, core = row // 8, (row // 2) % 4, row % 2
    row_peers = [lax.rem(col + step, 4) for step in (2, 1, 3)]
    col_peers = [
        row_index(lax.rem(x + dx, 4), lax.rem(z + dz, 4), lax.rem(core + dc, 2))
        for dx, dz, dc in plane_neighbours()
    ]

    barrier = pltpu.get_barrier_semaphore()
    for peer in row_peers:
        pl.semaphore_signal(barrier, inc=1, device_id=(row, peer), device_id_type=MESH)
    for peer in col_peers:
        pl.semaphore_signal(barrier, inc=1, device_id=(peer, col), device_id_type=MESH)

    total_one = jnp.float32(0)
    for block in range(sizes_one_ref.shape[0]):
        total_one = total_one + sizes_one_ref[block].astype(jnp.float32)
    total_two = jnp.float32(0)
    for block in range(sizes_two_ref.shape[0]):
        total_two = total_two + sizes_two_ref[block].astype(jnp.float32)
    log_one = jnp.log2(jnp.full((TILES, LANES), total_one, jnp.float32))
    log_two = jnp.log2(jnp.full((TILES, LANES), total_two, jnp.float32))
    size_one = sizes_one_ref[row]
    size_two = sizes_two_ref[col]
    slot = lax.broadcasted_iota(jnp.int32, (TILES, LANES), 0) * LANES + lax.broadcasted_iota(
        jnp.int32, (TILES, LANES), 1
    )
    live_row = slot < size_one
    live_col = slot < size_two

    scale = jnp.float32(2.0 / math.sqrt(mass_scale) * math.log2(math.e))
    for start in range(0, BLOCK, CHUNK):
        ids = lax.broadcasted_iota(jnp.int32, (CHUNK, BLOCK), 0) + start
        lanes = lax.broadcasted_iota(jnp.int32, (CHUNK, BLOCK), 1)
        both = (ids < size_one) & (lanes < size_two)
        rows = pl.ds(start, CHUNK)
        cost_ref[rows, :] = jnp.where(both, cross_ref[rows, :] * scale, jnp.float32(very_low))

    diag = diagonal()
    pl.semaphore_wait(barrier, 34)

    def exchange(box, mine, sweep, send, recv, targets):
        count = len(targets)
        for target in targets:
            pltpu.make_async_remote_copy(
                src_ref=box.at[sweep, mine],
                dst_ref=box.at[sweep, mine],
                send_sem=send.at[sweep],
                recv_sem=recv.at[sweep],
                device_id=target,
                device_id_type=MESH,
            ).start()
        everyone = box.at[sweep, pl.ds(0, count)]
        pltpu.make_async_copy(everyone, everyone, recv.at[sweep]).wait()
        parts = box[sweep]
        top = jnp.max(parts, axis=0)
        return top + jnp.log2(jnp.sum(jnp.exp2(parts - top[None]), axis=0))

    def sweep_body(sweep, gamma):
        for tile in range(TILES):
            column = []
            for start in range(tile * LANES, (tile + 1) * LANES, CHUNK):
                values = cost_ref[pl.ds(start, CHUNK), :] + gamma_row(gamma)
                top = jnp.max(values, axis=1, keepdims=True)
                summed = jnp.sum(jnp.exp2(values - top), axis=1, keepdims=True)
                column.append(jnp.broadcast_to(top + jnp.log2(summed), (CHUNK, LANES)))
            column = jnp.concatenate(column, axis=0)
            row_box[sweep, col, pl.ds(tile, 1), :] = jnp.sum(
                jnp.where(diag, column, 0.0), axis=0, keepdims=True
            )
        lse = exchange(
            row_box, col, sweep, row_send, row_recv, [(row, peer) for peer in row_peers]
        )
        rho = jnp.where(live_row, -log_one - lse, 0.0)
        row_ref[...] = rho
        for tile in range(TILES):
            spread = jnp.broadcast_to(rho[tile : tile + 1, :], (LANES, LANES))
            rho_ref[pl.ds(tile * LANES, LANES), :] = jnp.broadcast_to(
                jnp.sum(jnp.where(diag, spread, 0.0), axis=1, keepdims=True), (LANES, LANES)
            )
        for tile in range(TILES):
            lanes = pl.ds(tile * LANES, LANES)
            tops, sums = [], []
            for start in range(0, BLOCK, 2 * CHUNK):
                rows = pl.ds(start, 2 * CHUNK)
                values = (cost_ref[rows, lanes] + rho_ref[rows, :]).reshape(
                    2 * CHUNK // 8, 8, LANES
                )
                top = jnp.max(values, axis=0)
                tops.append(top)
                sums.append(jnp.sum(jnp.exp2(values - top[None]), axis=0))
            high = functools.reduce(jnp.maximum, tops)
            high = jnp.max(high, axis=0, keepdims=True)
            summed = sum(s * jnp.exp2(t - high) for s, t in zip(sums, tops))
            col_box[sweep, row, pl.ds(tile, 1), :] = high + jnp.log2(
                jnp.sum(summed, axis=0, keepdims=True)
            )
        lse = exchange(
            col_box, row, sweep, col_send, col_recv, [(peer, col) for peer in col_peers]
        )
        return jnp.where(live_col, -log_two - lse, 0.0)

    def gamma_row(gamma):
        return jnp.concatenate([gamma[t : t + 1, :] for t in range(TILES)], axis=1)

    gamma = lax.fori_loop(0, SWEEPS, sweep_body, jnp.zeros((TILES, LANES), jnp.float32))

    for start in range(0, BLOCK, CHUNK):
        rows = pl.ds(start, CHUNK)
        rho = rho_ref[rows, :]
        exponent = (
            cost_ref[rows, :] + jnp.concatenate([rho] * TILES, axis=1) + gamma_row(gamma)
        )
        plan_ref[rows, :] = jnp.float32(mass_scale) * jnp.exp2(exponent)
    unit = jnp.float32(math.log(2.0) / math.sqrt(mass_scale))
    row_ref[...] = jnp.where(live_row, row_ref[...] * unit + row_const_ref[...], 0.0)
    col_ref[...] = jnp.where(live_col, gamma * unit + col_const_ref[...], 0.0)

    def drain(sweep, carry):
        for box, send, count in ((row_box, row_send, 3), (col_box, col_send, 31)):
            everyone = box.at[sweep, pl.ds(0, count)]
            pltpu.make_async_copy(everyone, everyone, send.at[sweep]).wait()
        return carry

    lax.fori_loop(0, SWEEPS, drain, 0)


def sinkhorn(cross, row_const, col_const, sizes_one, sizes_two, mass_scale):
    vmem = pl.BlockSpec(memory_space=pltpu.VMEM)
    smem = pl.BlockSpec(memory_space=pltpu.SMEM)
    return pl.pallas_call(
        functools.partial(sinkhorn_kernel, mass_scale),
        out_shape=(
            jax.ShapeDtypeStruct((BLOCK, BLOCK), jnp.float32),
            jax.ShapeDtypeStruct((TILES, LANES), jnp.float32),
            jax.ShapeDtypeStruct((TILES, LANES), jnp.float32),
        ),
        in_specs=[vmem, vmem, vmem, smem, smem],
        out_specs=(vmem, vmem, vmem),
        scratch_shapes=[
            pltpu.VMEM((BLOCK, BLOCK), jnp.float32),
            pltpu.VMEM((BLOCK, LANES), jnp.float32),
            pltpu.VMEM((SWEEPS, 4, TILES, LANES), jnp.float32),
            pltpu.VMEM((SWEEPS, 32, TILES, LANES), jnp.float32),
            pltpu.SemaphoreType.DMA((SWEEPS,)),
            pltpu.SemaphoreType.DMA((SWEEPS,)),
            pltpu.SemaphoreType.DMA((SWEEPS,)),
            pltpu.SemaphoreType.DMA((SWEEPS,)),
        ],
        compiler_params=pltpu.CompilerParams(collective_id=0, has_side_effects=True),
        name="sinkhorn",
    )(cross, row_const, col_const, sizes_one, sizes_two)


def body(graph_one, graph_two, coupling, sizes_one, sizes_two):
    local_rows = graph_one.shape[0]
    count_one = graph_one.shape[1]
    local_cols = graph_two.shape[0]
    count_two = graph_two.shape[1]
    all_one = live_slots(sizes_one, count_one)
    all_two = live_slots(sizes_two, count_two)
    slots = jnp.arange(BLOCK, dtype=jnp.int32)
    live_rows = slots < sizes_one[lax.axis_index("row")]
    live_cols = slots < sizes_two[lax.axis_index("col")]
    total_one = jnp.sum(sizes_one).astype(jnp.float32)
    total_two = jnp.sum(sizes_two).astype(jnp.float32)
    live_both = live_rows[:, None] & live_cols[None, :]
    rounded_plan = jnp.where(live_both, coupling, jnp.float32(0.0)).astype(jnp.bfloat16)
    whole_plan = lax.all_gather(rounded_plan, "row", axis=0, tiled=True)
    first_product = jnp.dot(graph_one, whole_plan, preferred_element_type=jnp.float32).astype(
        jnp.bfloat16
    )
    whole_first = gather_directly(first_product, "col", 1)
    cross_term = lax.dot_general(
        whole_first, graph_two, (((1,), (1,)), ((), ())), preferred_element_type=jnp.float32
    )
    row_const = (
        jnp.sum(
            jnp.square(graph_one.astype(jnp.float32)) * all_one.astype(jnp.float32)[None, :], axis=1
        )
        / total_one
    )
    col_const = (
        jnp.sum(
            jnp.square(graph_two.astype(jnp.float32)) * all_two.astype(jnp.float32)[None, :], axis=1
        )
        / total_two
    )
    plan, row_potential, col_potential = sinkhorn(
        cross_term,
        row_const.reshape(TILES, LANES),
        col_const.reshape(TILES, LANES),
        sizes_one,
        sizes_two,
        float(count_one * count_two),
    )
    return plan, row_potential.reshape(local_rows), col_potential.reshape(local_cols)


def solution(mesh):
    return jax.shard_map(
        body,
        mesh=mesh,
        in_specs=(P("row", None), P("col", None), P("row", "col"), P(), P()),
        out_specs=(P("row", "col"), P("row"), P("col")),
        check_vma=False,
    )
```

```python
import functools
import math

import jax
import jax.numpy as jnp
from jax import lax
from jax.experimental import pallas as pl
from jax.experimental.pallas import tpu as pltpu
from jax.sharding import PartitionSpec as P

BLOCK = 512
SWEEPS = 5
LANES = 128
TILES = BLOCK // LANES
CHUNK = 64
WIDTHS = (256, 256)
STEPS = (
    (0, 0), (-1, 0), (1, 0), (0, -1), (0, 1), (2, 0), (-1, -1), (-1, 1),
    (1, -1), (1, 1), (0, 2), (2, -1), (2, 1), (-1, 2), (1, 2), (2, 2),
)
HALF = BLOCK // 2
UNIT = BLOCK // 4
MESH = pl.DeviceIdType.MESH

very_low = -1e30


def plane_neighbours():
    steps = []
    for dx in range(4):
        for dz in range(4):
            for dc in range(2):
                if dx or dz or dc:
                    far = min(dx, 4 - dx) + min(dz, 4 - dz)
                    steps.append((-far, -dc, dx, dz, dc))
    return [step[2:] for step in sorted(steps)]


def row_index(x, z, core):
    return (x * 4 + z) * 2 + core


def diagonal():
    return lax.broadcasted_iota(jnp.int32, (LANES, LANES), 0) == lax.broadcasted_iota(
        jnp.int32, (LANES, LANES), 1
    )


def gw_kernel(
    mass_scale,
    graph_one_ref,
    graph_two_ref,
    coupling_ref,
    sizes_one_ref,
    sizes_two_ref,
    cost_ref,
    rho_ref,
    vectors_ref,
    *scratch,
):
    parts = len(WIDTHS)
    plans, scratch = scratch[:parts], scratch[parts:]
    firsts, scratch = scratch[:parts], scratch[parts:]
    totals, scratch = scratch[:parts], scratch[parts:]
    (
        one_ref,
        two_ref,
        loaded_ref,
        squares_ref,
        row_box,
        col_box,
        load_sem,
        plan_send,
        plan_recv,
        pair_recv,
        first_send,
        first_recv,
        row_send,
        row_recv,
        col_send,
        col_recv,
    ) = scratch
    row = lax.axis_index("row")
    col = lax.axis_index("col")
    x, z, core = row // 8, (row // 2) % 4, row % 2
    partner = row + 1 - 2 * core
    row_peers = [lax.rem(col + step, 4) for step in (2, 1, 3)]
    col_peers = [
        row_index(lax.rem(x + dx, 4), lax.rem(z + dz, 4), lax.rem(core + dc, 2))
        for dx, dz, dc in plane_neighbours()
    ]

    barrier = pltpu.get_barrier_semaphore()
    for peer in row_peers:
        pl.semaphore_signal(barrier, inc=1, device_id=(row, peer), device_id_type=MESH)
    for peer in col_peers:
        pl.semaphore_signal(barrier, inc=1, device_id=(peer, col), device_id_type=MESH)

    load_coupling = pltpu.make_async_copy(coupling_ref, loaded_ref, load_sem.at[0])
    load_coupling.start()
    load_two = []
    for block in range(4):
        load_two.append(
            pltpu.make_async_copy(
                graph_two_ref.at[:, pl.ds(block * BLOCK, BLOCK)], two_ref.at[block], load_sem.at[1]
            )
        )
    load_one = []
    for block in range(32):
        load_one.append(
            pltpu.make_async_copy(
                graph_one_ref.at[:, pl.ds(block * BLOCK, BLOCK)], one_ref.at[block], load_sem.at[2]
            )
        )

    total_one = jnp.float32(0)
    for block in range(sizes_one_ref.shape[0]):
        total_one = total_one + sizes_one_ref[block].astype(jnp.float32)
    total_two = jnp.float32(0)
    for block in range(sizes_two_ref.shape[0]):
        total_two = total_two + sizes_two_ref[block].astype(jnp.float32)
    all_one = jnp.full((TILES, LANES), total_one, jnp.float32)
    all_two = jnp.full((TILES, LANES), total_two, jnp.float32)
    log_one = jnp.log2(all_one)
    log_two = jnp.log2(all_two)
    size_one = sizes_one_ref[row]
    size_two = sizes_two_ref[col]
    slot = lax.broadcasted_iota(jnp.int32, (TILES, LANES), 0) * LANES + lax.broadcasted_iota(
        jnp.int32, (TILES, LANES), 1
    )
    live_row = slot < size_one
    live_col = slot < size_two
    diag = diagonal()

    def live_part(start, width, offset=0):
        ids = lax.broadcasted_iota(jnp.int32, (CHUNK, width), 0) + start
        lanes = lax.broadcasted_iota(jnp.int32, (CHUNK, width), 1) + offset
        return (ids < size_one) & (lanes < size_two)

    load_coupling.wait()
    for copy in load_two + load_one:
        copy.start()
    for start in range(0, BLOCK, CHUNK):
        rows = pl.ds(start, CHUNK)
        offset = 0
        for part, width in enumerate(WIDTHS):
            kept = jnp.where(
                live_part(start, width, offset), loaded_ref[rows, pl.ds(offset, width)], 0.0
            )
            plans[part][row, rows, :] = kept.astype(jnp.bfloat16)
            offset += width
    squares_ref[...] = jnp.zeros_like(squares_ref)
    pl.semaphore_wait(barrier, 34)

    def place(half, first, second):
        dx, dz = (first, second) if half == 0 else (second, first)
        return row_index(lax.rem(x + dx + 4, 4), lax.rem(z + dz + 4, 4), core)

    def send_unit(part, step, half, turn, source, target):
        rows = pl.ds(half * HALF + turn * UNIT, UNIT)
        piece = plans[part].at[source, rows, :]
        pltpu.make_async_remote_copy(
            src_ref=piece,
            dst_ref=piece,
            send_sem=plan_send.at[part],
            recv_sem=plan_recv.at[part, step, half, turn],
            device_id=(target, col),
            device_id_type=MESH,
        ).start()

    def send_pair(part, step, half, source):
        piece = plans[part].at[source, pl.ds(half * HALF, HALF), :]
        pltpu.make_async_remote_copy(
            src_ref=piece,
            dst_ref=piece,
            send_sem=plan_send.at[part],
            recv_sem=pair_recv.at[part, step],
            device_id=(partner, col),
            device_id_type=MESH,
        ).start()

    def wait_bytes(ref, sem):
        pltpu.make_async_copy(ref, ref, sem).wait()

    def moves(part, step):
        first, second = STEPS[step]
        for half in range(2):
            source = place(half, first, second)
            for turn in range(2):
                if (first, second) != (0, 0):
                    rows = pl.ds(half * HALF + turn * UNIT, UNIT)
                    wait_bytes(
                        plans[part].at[source, rows, :], plan_recv.at[part, step, half, turn]
                    )
                onward = -1 if turn == 0 else 1
                if second == 0:
                    for sent in (-1, 1):
                        if first == 0 or (first == onward and sent == onward):
                            seen = sent if first == 0 else 2
                            send_unit(
                                part, STEPS.index((seen, 0)), half, turn, source,
                                place(half, -sent, 0),
                            )
                    for sent in (-1, 1):
                        send_unit(
                            part, STEPS.index((first, sent)), half, turn, source,
                            place(half, 0, -sent),
                        )
                elif second == onward:
                    send_unit(
                        part, STEPS.index((first, 2)), half, turn, source, place(half, 0, -onward)
                    )
            send_pair(part, step, half, source)

    def offset_of(step, axis):
        value = jnp.int32(STEPS[-1][axis])
        for index in range(len(STEPS) - 1):
            value = jnp.where(step == index, jnp.int32(STEPS[index][axis]), value)
        return value

    def multiply(part, step, parity):
        first, second = offset_of(step, 0), offset_of(step, 1)
        for half in range(2):
            source = place(half, first, second)
            source = source + parity * (1 - 2 * core)
            rows = pl.ds(half * HALF, HALF)
            left = one_ref[source, :, rows]
            totals[part][...] += jnp.dot(
                left, plans[part][source, rows, :], preferred_element_type=jnp.float32
            )
            if part == 0:
                size = sizes_one_ref[source]
                for start in range(0, BLOCK, CHUNK):
                    squares = squares_ref[pl.ds(start, CHUNK), :]
                    for tile in range(2):
                        lanes = half * HALF + tile * LANES
                        ids = lax.broadcasted_iota(jnp.int32, (CHUNK, LANES), 1) + lanes
                        value = one_ref[source, pl.ds(start, CHUNK), pl.ds(lanes, LANES)].astype(
                            jnp.float32
                        )
                        squares = squares + jnp.where(ids < size, value * value, 0.0)
                    squares_ref[pl.ds(start, CHUNK), :] = squares

    def first_copy(part, half, source, key, target):
        piece = firsts[part].at[source, pl.ds(half * HALF, HALF), :]
        return pltpu.make_async_remote_copy(
            src_ref=piece,
            dst_ref=piece,
            send_sem=first_send.at[part],
            recv_sem=first_recv.at[part, key],
            device_id=(row, target),
            device_id_type=MESH,
        )

    up, down, across = lax.rem(col + 1, 4), lax.rem(col + 3, 4), lax.rem(col + 2, 4)

    def first_start(part):
        for start in range(0, BLOCK, CHUNK):
            rows = pl.ds(start, CHUNK)
            firsts[part][col, rows, :] = totals[part][rows, :].astype(jnp.bfloat16)
        first_copy(part, 0, col, 0, up).start()
        first_copy(part, 1, col, 1, down).start()
        first_copy(part, 1, col, 2, up).start()
        first_copy(part, 0, col, 3, down).start()

    def first_wait(part, half, source, key):
        wait_bytes(firsts[part].at[source, pl.ds(half * HALF, HALF), :], first_recv.at[part, key])

    def first_onward(part):
        first_wait(part, 0, down, 0)
        first_copy(part, 0, down, 4, up).start()
        first_wait(part, 1, up, 1)
        first_copy(part, 1, up, 5, down).start()

    def cross_add(part, source, fresh=False):
        offset = sum(WIDTHS[:part])
        added = lax.dot_general(
            firsts[part][source],
            two_ref[source, :, pl.ds(offset, WIDTHS[part])],
            (((1,), (1,)), ((), ())),
            preferred_element_type=jnp.float32,
        )
        if fresh:
            cost_ref[...] = added
        else:
            cost_ref[...] += added

    def first_end(part):
        cross_add(part, col, fresh=part == 0)
        first_wait(part, 1, down, 2)
        cross_add(part, down)
        first_wait(part, 0, up, 3)
        cross_add(part, up)
        first_wait(part, 0, across, 4)
        first_wait(part, 1, across, 5)
        cross_add(part, across)

    last = len(STEPS) - 1
    for part in range(parts):
        totals[part][...] = jnp.zeros_like(totals[part])
    moves(0, 0)
    if parts > 1:
        moves(1, 0)
    wait_bytes(two_ref, load_sem.at[1])
    col_square = []
    for tile in range(TILES):
        summed = []
        for start in range(tile * LANES, (tile + 1) * LANES, CHUNK):
            gathered = jnp.zeros((CHUNK, LANES), jnp.float32)
            for block in range(4):
                for lane in range(TILES):
                    ids = lax.broadcasted_iota(jnp.int32, (CHUNK, LANES), 1) + lane * LANES
                    value = two_ref[block, pl.ds(start, CHUNK), pl.ds(lane * LANES, LANES)].astype(
                        jnp.float32
                    )
                    gathered = gathered + jnp.where(
                        ids < sizes_two_ref[block], value * value, 0.0
                    )
            summed.append(
                jnp.broadcast_to(jnp.sum(gathered, axis=1, keepdims=True), (CHUNK, LANES))
            )
        vectors_ref[pl.ds(12 + tile, 1), :] = jnp.sum(
            jnp.where(diag, jnp.concatenate(summed, axis=0), 0.0), axis=0, keepdims=True
        )
    wait_bytes(one_ref, load_sem.at[2])

    for part in range(parts):

        def one_step(step, carry, part=part):
            for index in range(1, len(STEPS)):

                @pl.when(step == index)
                def _():
                    moves(part, index)
                    if index == 6 and 1 < part + 1 < parts:
                        moves(part + 1, 0)
                    if part and index == 5:
                        first_onward(part - 1)
                    if part and index == 11:
                        first_end(part - 1)

            multiply(part, step, 0)

            @pl.when(step > 0)
            def _():
                wait_bytes(plans[part].at[0], pair_recv.at[part, lax.max(step - 1, 0)])
                multiply(part, lax.max(step - 1, 0), 1)

            return carry

        lax.fori_loop(0, len(STEPS), one_step, 0)
        wait_bytes(plans[part].at[0], pair_recv.at[part, last])
        multiply(part, last, 1)
        first_start(part)
    first_onward(parts - 1)
    for tile in range(TILES):
        column = jnp.broadcast_to(
            jnp.sum(squares_ref[pl.ds(tile * LANES, LANES), :], axis=1, keepdims=True),
            (LANES, LANES),
        )
        vectors_ref[pl.ds(8 + tile, 1), :] = jnp.sum(
            jnp.where(diag, column, 0.0), axis=0, keepdims=True
        )
    first_end(parts - 1)

    scale = jnp.float32(2.0 / math.sqrt(mass_scale) * math.log2(math.e))
    for start in range(0, BLOCK, CHUNK):
        rows = pl.ds(start, CHUNK)
        cost_ref[rows, :] = jnp.where(
            live_part(start, BLOCK), cost_ref[rows, :] * scale, jnp.float32(very_low)
        )

    def exchange(box, mine, sweep, send, recv, targets):
        for target in targets:
            pltpu.make_async_remote_copy(
                src_ref=box.at[sweep, mine],
                dst_ref=box.at[sweep, mine],
                send_sem=send.at[sweep],
                recv_sem=recv.at[sweep],
                device_id=target,
                device_id_type=MESH,
            ).start()
        wait_bytes(box.at[sweep, pl.ds(0, len(targets))], recv.at[sweep])
        logs = box[sweep]
        top = jnp.max(logs, axis=0)
        return top + jnp.log2(jnp.sum(jnp.exp2(logs - top[None]), axis=0))

    def gamma_row(gamma):
        return jnp.concatenate([gamma[t : t + 1, :] for t in range(TILES)], axis=1)

    def sweep_body(sweep, gamma):
        for tile in range(TILES):
            column = []
            for start in range(tile * LANES, (tile + 1) * LANES, CHUNK):
                values = cost_ref[pl.ds(start, CHUNK), :] + gamma_row(gamma)
                top = jnp.max(values, axis=1, keepdims=True)
                summed = jnp.sum(jnp.exp2(values - top), axis=1, keepdims=True)
                column.append(jnp.broadcast_to(top + jnp.log2(summed), (CHUNK, LANES)))
            column = jnp.concatenate(column, axis=0)
            row_box[sweep, col, pl.ds(tile, 1), :] = jnp.sum(
                jnp.where(diag, column, 0.0), axis=0, keepdims=True
            )
        lse = exchange(
            row_box, col, sweep, row_send, row_recv, [(row, peer) for peer in row_peers]
        )
        rho = jnp.where(live_row, -log_one - lse, 0.0)
        vectors_ref[pl.ds(0, TILES), :] = rho
        for tile in range(TILES):
            spread = jnp.broadcast_to(rho[tile : tile + 1, :], (LANES, LANES))
            rho_ref[pl.ds(tile * LANES, LANES), :] = jnp.broadcast_to(
                jnp.sum(jnp.where(diag, spread, 0.0), axis=1, keepdims=True), (LANES, LANES)
            )
        for tile in range(TILES):
            lanes = pl.ds(tile * LANES, LANES)
            tops, sums = [], []
            for start in range(0, BLOCK, 2 * CHUNK):
                rows = pl.ds(start, 2 * CHUNK)
                values = (cost_ref[rows, lanes] + rho_ref[rows, :]).reshape(
                    2 * CHUNK // 8, 8, LANES
                )
                top = jnp.max(values, axis=0)
                tops.append(top)
                sums.append(jnp.sum(jnp.exp2(values - top[None]), axis=0))
            high = functools.reduce(jnp.maximum, tops)
            high = jnp.max(high, axis=0, keepdims=True)
            summed = sum(s * jnp.exp2(t - high) for s, t in zip(sums, tops))
            col_box[sweep, row, pl.ds(tile, 1), :] = high + jnp.log2(
                jnp.sum(summed, axis=0, keepdims=True)
            )
        lse = exchange(
            col_box, row, sweep, col_send, col_recv, [(peer, col) for peer in col_peers]
        )
        return jnp.where(live_col, -log_two - lse, 0.0)

    gamma = lax.fori_loop(0, SWEEPS, sweep_body, jnp.zeros((TILES, LANES), jnp.float32))

    unit = jnp.float32(math.log(2.0) / math.sqrt(mass_scale))
    rho = vectors_ref[pl.ds(0, TILES), :]
    row_const = vectors_ref[pl.ds(8, TILES), :] / all_one
    col_const = vectors_ref[pl.ds(12, TILES), :] / all_two
    vectors_ref[pl.ds(4, TILES), :] = gamma
    vectors_ref[pl.ds(8, TILES), :] = jnp.where(live_row, rho * unit + row_const, 0.0)
    vectors_ref[pl.ds(12, TILES), :] = jnp.where(live_col, gamma * unit + col_const, 0.0)

    def drain(sweep, carry):
        for box, send, count in ((row_box, row_send, 3), (col_box, col_send, 31)):
            wait_bytes(box.at[sweep, pl.ds(0, count)], send.at[sweep])
        return carry

    lax.fori_loop(0, SWEEPS, drain, 0)
    for part in range(parts):
        wait_bytes(plans[part].at[pl.ds(0, 31)], plan_send.at[part])
        wait_bytes(firsts[part].at[pl.ds(0, 3)], first_send.at[part])


def finish_kernel(mass_scale, cost_ref, rho_ref, vectors_ref, plan_ref, row_ref, col_ref):
    gamma = jnp.concatenate([vectors_ref[pl.ds(4 + t, 1), :] for t in range(TILES)], axis=1)
    for start in range(0, BLOCK, CHUNK):
        rows = pl.ds(start, CHUNK)
        exponent = (
            cost_ref[rows, :] + jnp.concatenate([rho_ref[rows, :]] * TILES, axis=1) + gamma
        )
        plan_ref[rows, :] = jnp.float32(mass_scale) * jnp.exp2(exponent)
    row_ref[...] = vectors_ref[pl.ds(8, TILES), :]
    col_ref[...] = vectors_ref[pl.ds(12, TILES), :]


def body(graph_one, graph_two, coupling, sizes_one, sizes_two):
    mass_scale = float(graph_one.shape[1] * graph_two.shape[1])
    vmem = pl.BlockSpec(memory_space=pltpu.VMEM)
    smem = pl.BlockSpec(memory_space=pltpu.SMEM)
    hbm = pl.BlockSpec(memory_space=pltpu.HBM)
    parts = len(WIDTHS)
    f32, bf16 = jnp.float32, jnp.bfloat16
    dma = pltpu.SemaphoreType.DMA
    cost, rho, vectors = pl.pallas_call(
        functools.partial(gw_kernel, mass_scale),
        out_shape=(
            jax.ShapeDtypeStruct((BLOCK, BLOCK), f32),
            jax.ShapeDtypeStruct((BLOCK, LANES), f32),
            jax.ShapeDtypeStruct((4 * TILES, LANES), f32),
        ),
        in_specs=[hbm, hbm, hbm, smem, smem],
        out_specs=(vmem, vmem, vmem),
        scratch_shapes=[
            *(pltpu.VMEM((32, BLOCK, width), bf16) for width in WIDTHS),
            *(pltpu.VMEM((4, BLOCK, width), bf16) for width in WIDTHS),
            *(pltpu.VMEM((BLOCK, width), f32) for width in WIDTHS),
            pltpu.VMEM((32, BLOCK, BLOCK), bf16),
            pltpu.VMEM((4, BLOCK, BLOCK), bf16),
            pltpu.VMEM((BLOCK, BLOCK), f32),
            pltpu.VMEM((BLOCK, LANES), f32),
            pltpu.VMEM((SWEEPS, 4, TILES, LANES), f32),
            pltpu.VMEM((SWEEPS, 32, TILES, LANES), f32),
            dma((3,)),
            dma((parts,)),
            dma((parts, len(STEPS), 2, 2)),
            dma((parts, len(STEPS))),
            dma((parts,)),
            dma((parts, 6)),
            dma((SWEEPS,)),
            dma((SWEEPS,)),
            dma((SWEEPS,)),
            dma((SWEEPS,)),
        ],
        compiler_params=pltpu.CompilerParams(
            collective_id=0, has_side_effects=True, vmem_limit_bytes=56 * 1024 * 1024
        ),
        name="gw_step",
    )(graph_one, graph_two, coupling, sizes_one, sizes_two)
    plan, row_potential, col_potential = pl.pallas_call(
        functools.partial(finish_kernel, mass_scale),
        out_shape=(
            jax.ShapeDtypeStruct((BLOCK, BLOCK), f32),
            jax.ShapeDtypeStruct((TILES, LANES), f32),
            jax.ShapeDtypeStruct((TILES, LANES), f32),
        ),
        in_specs=[vmem, vmem, vmem],
        out_specs=(vmem, vmem, vmem),
        name="finish",
    )(cost, rho, vectors)
    return plan, row_potential.reshape(BLOCK), col_potential.reshape(BLOCK)


def solution(mesh):
    return jax.shard_map(
        body,
        mesh=mesh,
        in_specs=(P("row", None), P("col", None), P("row", "col"), P(), P()),
        out_specs=(P("row", "col"), P("row"), P("col")),
        check_vma=False,
    )
```

```python
import functools
import math

import jax
import jax.numpy as jnp
from jax import lax
from jax.experimental import pallas as pl
from jax.experimental.pallas import tpu as pltpu
from jax.sharding import PartitionSpec as P

BLOCK = 512
SWEEPS = 5
LANES = 128
TILES = BLOCK // LANES
CHUNK = 64
WIDTH = 256
PARTS = BLOCK // WIDTH
OFFSETS = (0, -1, 1, 2)
STEPS = tuple((first, second) for second in OFFSETS for first in OFFSETS)
HALF = BLOCK // 2
UNIT = BLOCK // 4
MESH = pl.DeviceIdType.MESH

very_low = -1e30


def plane_neighbours():
    steps = []
    for dx in range(4):
        for dz in range(4):
            for dc in range(2):
                if dx or dz or dc:
                    far = min(dx, 4 - dx) + min(dz, 4 - dz)
                    steps.append((-far, -dc, dx, dz, dc))
    return [step[2:] for step in sorted(steps)]


def diagonal():
    return lax.broadcasted_iota(jnp.int32, (LANES, LANES), 0) == lax.broadcasted_iota(
        jnp.int32, (LANES, LANES), 1
    )


UNIT_US, HOP_US, SLOT_US, AHEAD_US = 1.405, 2.5, 1.0, 2.8


def sends_of(part, half, turn, first, second):
    onward = 1 if turn == 0 else -1
    out = []
    if second == 0:
        if first == 0:
            for way in (1, -1):
                out.append((0, way, (-way, 0), 4 if way == onward else 3))
        elif first == -onward:
            out.append((0, onward, (2, 0), 3))
        for way in (1, -1):
            out.append((1, way, (first, -way), 2 if way == onward else 1))
    elif second == -onward:
        out.append((1, onward, (first, 2), 1))
    return out


def timetable():
    arrival = {
        (part, half, turn, 0, 0): 0.0
        for part in range(PARTS)
        for half in range(2)
        for turn in range(2)
    }
    free = {(axis, way): 0.0 for axis in range(2) for way in (1, -1)}
    pending, known, slots, now = [], set(), [], 0.0
    while len(known) < PARTS * 4 * len(STEPS):
        fresh = sorted(
            (unit for unit in arrival if arrival[unit] <= now and unit not in known),
            key=lambda unit: (arrival[unit], unit),
        )
        known.update(fresh)
        for unit in fresh:
            pending += [(unit, *send) for send in sends_of(*unit)]
        sends = []
        for axis, way in free:
            while max(free[axis, way], now) - now < AHEAD_US:
                ready = [
                    send
                    for send in pending
                    if send[2] == way and (send[1] + send[0][1]) % 2 == axis
                ]
                if not ready:
                    break
                best = min(ready, key=lambda send: (send[0][0], -send[4]))
                pending.remove(best)
                free[axis, way] = max(free[axis, way], now) + UNIT_US
                arrival[best[0][:3] + best[3]] = free[axis, way] + HOP_US
                sends.append(best)
        slots.append((fresh, sends))
        now += SLOT_US
    return slots


def items_of(slots):
    count, work, last = {}, {}, -1
    for index, (fresh, _) in enumerate(slots):
        for part, _, _, first, second in fresh:
            key = (part, STEPS.index((first, second)))
            count[key] = count.get(key, 0) + 1
            if count[key] == 4:
                last = max(index + 2, last + 1)
                work[last] = key
    return work


def gw_kernel(
    mass_scale,
    graph_one_ref,
    graph_two_ref,
    coupling_ref,
    sizes_one_ref,
    sizes_two_ref,
    cost_ref,
    rho_ref,
    vectors_ref,
    *scratch,
):
    (
        plans,
        firsts,
        totals,
        one_ref,
        two_ref,
        loaded_ref,
        squares_ref,
        row_box,
        col_box,
        load_sem,
        plan_send,
        plan_recv,
        pair_recv,
        first_send,
        first_recv,
        row_send,
        row_recv,
        col_send,
        col_recv,
    ) = scratch
    row = lax.axis_index("row")
    col = lax.axis_index("col")
    x, z, core = row // 8, (row // 2) % 4, row % 2
    other = 1 - core
    partner = row + 1 - 2 * core

    def around(value):
        return [value] + [
            jnp.where(value >= 4 - step, value + step - 4, value + step) for step in (1, 2, 3)
        ]

    xs, zs = [8 * value for value in around(x)], [2 * value for value in around(z)]
    _, up, across, down = around(col)
    row_peers = [across, up, down]
    col_peers = [
        xs[dx] + zs[dz] + (other if dc else core) for dx, dz, dc in plane_neighbours()
    ]
    places = [[xs[dx] + zs[dz] + core for dz in range(4)] for dx in range(4)]

    barrier = pltpu.get_barrier_semaphore()
    for peer in row_peers:
        pl.semaphore_signal(barrier, inc=1, device_id=(row, peer), device_id_type=MESH)
    for peer in col_peers:
        pl.semaphore_signal(barrier, inc=1, device_id=(peer, col), device_id_type=MESH)

    load_coupling = pltpu.make_async_copy(coupling_ref, loaded_ref, load_sem.at[0])
    load_coupling.start()
    load_two = []
    for block in range(4):
        load_two.append(
            pltpu.make_async_copy(
                graph_two_ref.at[:, pl.ds(block * BLOCK, BLOCK)], two_ref.at[block], load_sem.at[1]
            )
        )
    load_one = []
    for block in range(32):
        load_one.append(
            pltpu.make_async_copy(
                graph_one_ref.at[:, pl.ds(block * BLOCK, BLOCK)], one_ref.at[block], load_sem.at[2]
            )
        )

    total_one = jnp.float32(0)
    for block in range(sizes_one_ref.shape[0]):
        total_one = total_one + sizes_one_ref[block].astype(jnp.float32)
    total_two = jnp.float32(0)
    for block in range(sizes_two_ref.shape[0]):
        total_two = total_two + sizes_two_ref[block].astype(jnp.float32)
    all_one = jnp.full((TILES, LANES), total_one, jnp.float32)
    all_two = jnp.full((TILES, LANES), total_two, jnp.float32)
    log_one = jnp.log2(all_one)
    log_two = jnp.log2(all_two)
    size_one = sizes_one_ref[row]
    size_two = sizes_two_ref[col]
    slot = lax.broadcasted_iota(jnp.int32, (TILES, LANES), 0) * LANES + lax.broadcasted_iota(
        jnp.int32, (TILES, LANES), 1
    )
    live_row = slot < size_one
    live_col = slot < size_two
    diag = diagonal()

    def live_part(start, width, offset=0):
        ids = lax.broadcasted_iota(jnp.int32, (CHUNK, width), 0) + start
        lanes = lax.broadcasted_iota(jnp.int32, (CHUNK, width), 1) + offset
        return (ids < size_one) & (lanes < size_two)

    load_coupling.wait()
    for copy in load_two + load_one:
        copy.start()
    for start in range(0, BLOCK, CHUNK):
        rows = pl.ds(start, CHUNK)
        for part in range(PARTS):
            kept = jnp.where(
                live_part(start, WIDTH, part * WIDTH),
                loaded_ref[rows, pl.ds(part * WIDTH, WIDTH)],
                0.0,
            )
            plans[part, row, rows, :] = kept.astype(jnp.bfloat16)
    squares_ref[...] = jnp.zeros_like(squares_ref)
    pl.semaphore_wait(barrier, 34)

    def place(half, first, second):
        dx, dz = (first, second) if half == 0 else (second, first)
        return places[dx % 4][dz % 4]

    def wait_bytes(ref, sem):
        pltpu.make_async_copy(ref, ref, sem).wait()

    def piece_of(part, half, turn, first, second):
        rows = pl.ds(half * HALF + turn * UNIT, UNIT)
        return plans.at[part, place(half, first, second), rows, :]

    def moves(fresh, sends):
        for unit in fresh:
            part, half, turn, first, second = unit
            step = STEPS.index((first, second))
            piece = piece_of(*unit)
            if (first, second) != (0, 0):
                wait_bytes(piece, plan_recv.at[part, step, half, turn])
        for unit, axis, way, seen, _ in sends:
            part, half, turn, first, second = unit
            piece = piece_of(*unit)
            target = place(half, way, 0) if axis == 0 else place(half, 0, way)
            pltpu.make_async_remote_copy(
                src_ref=piece,
                dst_ref=piece,
                send_sem=plan_send.at[part],
                recv_sem=plan_recv.at[part, STEPS.index(seen), half, turn],
                device_id=(target, col),
                device_id_type=MESH,
            ).start()
        for unit in fresh:
            part, half, turn, first, second = unit
            piece = piece_of(*unit)
            pltpu.make_async_remote_copy(
                src_ref=piece,
                dst_ref=piece,
                send_sem=plan_send.at[part],
                recv_sem=pair_recv.at[part, STEPS.index((first, second))],
                device_id=(partner, col),
                device_id_type=MESH,
            ).start()

    def pick(options, index):
        value = options[OFFSETS[-1] % 4]
        for place_of, offset in enumerate(OFFSETS[:-1]):
            value = jnp.where(index == place_of, options[offset % 4], value)
        return value

    def multiply(code):
        part = jnp.where(code >= len(STEPS), 1, 0)
        step = code - len(STEPS) * part
        second = (
            jnp.where(step >= 4, 1, 0) + jnp.where(step >= 8, 1, 0) + jnp.where(step >= 12, 1, 0)
        )
        first = step - 4 * second
        wait_bytes(plans.at[0, 0], pair_recv.at[part, step])
        chips = (pick(xs, first) + pick(zs, second), pick(xs, second) + pick(zs, first))
        for start in range(0, BLOCK, HALF):
            total = totals[part, pl.ds(start, HALF), :]
            for half in range(2):
                rows = pl.ds(half * HALF, HALF)
                for owner in (core, other):
                    source = chips[half] + owner
                    total = total + jnp.dot(
                        one_ref[source, pl.ds(start, HALF), rows],
                        plans[part, source, rows, :],
                        preferred_element_type=jnp.float32,
                    )
            totals[part, pl.ds(start, HALF), :] = total

        @pl.when(part == 0)
        def _():
            for start in range(0, BLOCK, CHUNK):
                squares = squares_ref[pl.ds(start, CHUNK), :]
                for half in range(2):
                    for owner in (core, other):
                        source = chips[half] + owner
                        size = sizes_one_ref[source]
                        for tile in range(2):
                            lanes = half * HALF + tile * LANES
                            ids = lax.broadcasted_iota(jnp.int32, (CHUNK, LANES), 1) + lanes
                            value = one_ref[
                                source, pl.ds(start, CHUNK), pl.ds(lanes, LANES)
                            ].astype(jnp.float32)
                            squares = squares + jnp.where(ids < size, value * value, 0.0)
                squares_ref[pl.ds(start, CHUNK), :] = squares

    def first_copy(part, half, source, key, target):
        piece = firsts.at[part, source, pl.ds(half * HALF, HALF), :]
        return pltpu.make_async_remote_copy(
            src_ref=piece,
            dst_ref=piece,
            send_sem=first_send.at[part],
            recv_sem=first_recv.at[part, key],
            device_id=(row, target),
            device_id_type=MESH,
        )

    def first_start(part):
        for start in range(0, BLOCK, CHUNK):
            rows = pl.ds(start, CHUNK)
            firsts[part, col, rows, :] = totals[part, rows, :].astype(jnp.bfloat16)
        first_copy(part, 0, col, 0, up).start()
        first_copy(part, 1, col, 1, down).start()
        first_copy(part, 1, col, 2, up).start()
        first_copy(part, 0, col, 3, down).start()

    def first_wait(part, half, source, key):
        wait_bytes(firsts.at[part, source, pl.ds(half * HALF, HALF), :], first_recv.at[part, key])

    def first_onward(part):
        first_wait(part, 0, down, 0)
        first_copy(part, 0, down, 4, up).start()
        first_wait(part, 1, up, 1)
        first_copy(part, 1, up, 5, down).start()

    def cross_add(part, source, fresh=False):
        added = lax.dot_general(
            firsts[part, source],
            two_ref[source, :, pl.ds(part * WIDTH, WIDTH)],
            (((1,), (1,)), ((), ())),
            preferred_element_type=jnp.float32,
        )
        if fresh:
            cost_ref[...] = added
        else:
            cost_ref[...] += added

    def first_end(part):
        cross_add(part, col, fresh=part == 0)
        first_wait(part, 1, down, 2)
        cross_add(part, down)
        first_wait(part, 0, up, 3)
        cross_add(part, up)
        first_wait(part, 0, across, 4)
        first_wait(part, 1, across, 5)
        cross_add(part, across)

    slots = timetable()
    work = items_of(slots)
    length = max(work) + 1
    slots = slots + [([], [])] * (length - len(slots))
    whole = [max(slot for slot in work if work[slot][0] == part) for part in range(PARTS)]
    extra = {}
    for part in range(PARTS - 1):
        extra[whole[part] + 1] = [functools.partial(first_start, part)]
        extra[whole[part] + 8] = [functools.partial(first_onward, part)]
        extra[whole[part] + 16] = [functools.partial(first_end, part)]
    totals[...] = jnp.zeros_like(totals)
    moves(*slots[0])
    wait_bytes(two_ref, load_sem.at[1])
    col_square = []
    for tile in range(TILES):
        summed = []
        for start in range(tile * LANES, (tile + 1) * LANES, CHUNK):
            gathered = jnp.zeros((CHUNK, LANES), jnp.float32)
            for block in range(4):
                for lane in range(TILES):
                    ids = lax.broadcasted_iota(jnp.int32, (CHUNK, LANES), 1) + lane * LANES
                    value = two_ref[block, pl.ds(start, CHUNK), pl.ds(lane * LANES, LANES)].astype(
                        jnp.float32
                    )
                    gathered = gathered + jnp.where(
                        ids < sizes_two_ref[block], value * value, 0.0
                    )
            summed.append(
                jnp.broadcast_to(jnp.sum(gathered, axis=1, keepdims=True), (CHUNK, LANES))
            )
        vectors_ref[pl.ds(12 + tile, 1), :] = jnp.sum(
            jnp.where(diag, jnp.concatenate(summed, axis=0), 0.0), axis=0, keepdims=True
        )
    wait_bytes(one_ref, load_sem.at[2])

    def one_slot(slot, carry):
        for group in range(0, length, 8):

            @pl.when((slot >= group) & (slot < group + 8))
            def _():
                for index in range(max(group, 1), min(group + 8, length)):
                    if slots[index] != ([], []) or index in extra:

                        @pl.when(slot == index)
                        def _():
                            moves(*slots[index])
                            for run in extra.get(index, ()):
                                run()

        code = jnp.int32(-1)
        for index, (part, step) in work.items():
            code = jnp.where(slot == index, part * len(STEPS) + step, code)

        @pl.when(code >= 0)
        def _():
            multiply(code)

        return carry

    lax.fori_loop(0, length, one_slot, 0)
    first_start(PARTS - 1)
    first_onward(PARTS - 1)
    for tile in range(TILES):
        column = jnp.broadcast_to(
            jnp.sum(squares_ref[pl.ds(tile * LANES, LANES), :], axis=1, keepdims=True),
            (LANES, LANES),
        )
        vectors_ref[pl.ds(8 + tile, 1), :] = jnp.sum(
            jnp.where(diag, column, 0.0), axis=0, keepdims=True
        )
    first_end(PARTS - 1)

    scale = jnp.float32(2.0 / math.sqrt(mass_scale) * math.log2(math.e))
    for start in range(0, BLOCK, CHUNK):
        rows = pl.ds(start, CHUNK)
        cost_ref[rows, :] = jnp.where(
            live_part(start, BLOCK), cost_ref[rows, :] * scale, jnp.float32(very_low)
        )

    def exchange(box, mine, sweep, send, recv, targets):
        for target in targets:
            pltpu.make_async_remote_copy(
                src_ref=box.at[sweep, mine],
                dst_ref=box.at[sweep, mine],
                send_sem=send.at[sweep],
                recv_sem=recv.at[sweep],
                device_id=target,
                device_id_type=MESH,
            ).start()
        wait_bytes(box.at[sweep, pl.ds(0, len(targets))], recv.at[sweep])
        logs = box[sweep]
        top = jnp.max(logs, axis=0)
        return top + jnp.log2(jnp.sum(jnp.exp2(logs - top[None]), axis=0))

    def gamma_row(gamma):
        return jnp.concatenate([gamma[t : t + 1, :] for t in range(TILES)], axis=1)

    def sweep_body(sweep, gamma):
        for tile in range(TILES):
            column = []
            for start in range(tile * LANES, (tile + 1) * LANES, CHUNK):
                values = cost_ref[pl.ds(start, CHUNK), :] + gamma_row(gamma)
                top = jnp.max(values, axis=1, keepdims=True)
                summed = jnp.sum(jnp.exp2(values - top), axis=1, keepdims=True)
                column.append(jnp.broadcast_to(top + jnp.log2(summed), (CHUNK, LANES)))
            column = jnp.concatenate(column, axis=0)
            row_box[sweep, col, pl.ds(tile, 1), :] = jnp.sum(
                jnp.where(diag, column, 0.0), axis=0, keepdims=True
            )
        lse = exchange(
            row_box, col, sweep, row_send, row_recv, [(row, peer) for peer in row_peers]
        )
        rho = jnp.where(live_row, -log_one - lse, 0.0)
        vectors_ref[pl.ds(0, TILES), :] = rho
        for tile in range(TILES):
            spread = jnp.broadcast_to(rho[tile : tile + 1, :], (LANES, LANES))
            rho_ref[pl.ds(tile * LANES, LANES), :] = jnp.broadcast_to(
                jnp.sum(jnp.where(diag, spread, 0.0), axis=1, keepdims=True), (LANES, LANES)
            )
        for tile in range(TILES):
            lanes = pl.ds(tile * LANES, LANES)
            tops, sums = [], []
            for start in range(0, BLOCK, 2 * CHUNK):
                rows = pl.ds(start, 2 * CHUNK)
                values = (cost_ref[rows, lanes] + rho_ref[rows, :]).reshape(
                    2 * CHUNK // 8, 8, LANES
                )
                top = jnp.max(values, axis=0)
                tops.append(top)
                sums.append(jnp.sum(jnp.exp2(values - top[None]), axis=0))
            high = functools.reduce(jnp.maximum, tops)
            high = jnp.max(high, axis=0, keepdims=True)
            summed = sum(s * jnp.exp2(t - high) for s, t in zip(sums, tops))
            col_box[sweep, row, pl.ds(tile, 1), :] = high + jnp.log2(
                jnp.sum(summed, axis=0, keepdims=True)
            )
        lse = exchange(
            col_box, row, sweep, col_send, col_recv, [(peer, col) for peer in col_peers]
        )
        return jnp.where(live_col, -log_two - lse, 0.0)

    gamma = lax.fori_loop(0, SWEEPS, sweep_body, jnp.zeros((TILES, LANES), jnp.float32))

    unit = jnp.float32(math.log(2.0) / math.sqrt(mass_scale))
    rho = vectors_ref[pl.ds(0, TILES), :]
    row_const = vectors_ref[pl.ds(8, TILES), :] / all_one
    col_const = vectors_ref[pl.ds(12, TILES), :] / all_two
    vectors_ref[pl.ds(4, TILES), :] = gamma
    vectors_ref[pl.ds(8, TILES), :] = jnp.where(live_row, rho * unit + row_const, 0.0)
    vectors_ref[pl.ds(12, TILES), :] = jnp.where(live_col, gamma * unit + col_const, 0.0)

    def drain(sweep, carry):
        for box, send, count in ((row_box, row_send, 3), (col_box, col_send, 31)):
            wait_bytes(box.at[sweep, pl.ds(0, count)], send.at[sweep])
        return carry

    lax.fori_loop(0, SWEEPS, drain, 0)
    for part in range(PARTS):
        wait_bytes(plans.at[part, pl.ds(0, 31)], plan_send.at[part])
        wait_bytes(firsts.at[part, pl.ds(0, 3)], first_send.at[part])


def finish_kernel(mass_scale, cost_ref, rho_ref, vectors_ref, plan_ref, row_ref, col_ref):
    gamma = jnp.concatenate([vectors_ref[pl.ds(4 + t, 1), :] for t in range(TILES)], axis=1)
    for start in range(0, BLOCK, CHUNK):
        rows = pl.ds(start, CHUNK)
        exponent = (
            cost_ref[rows, :] + jnp.concatenate([rho_ref[rows, :]] * TILES, axis=1) + gamma
        )
        plan_ref[rows, :] = jnp.float32(mass_scale) * jnp.exp2(exponent)
    row_ref[...] = vectors_ref[pl.ds(8, TILES), :]
    col_ref[...] = vectors_ref[pl.ds(12, TILES), :]


def body(graph_one, graph_two, coupling, sizes_one, sizes_two):
    mass_scale = float(graph_one.shape[1] * graph_two.shape[1])
    vmem = pl.BlockSpec(memory_space=pltpu.VMEM)
    smem = pl.BlockSpec(memory_space=pltpu.SMEM)
    hbm = pl.BlockSpec(memory_space=pltpu.HBM)
    f32, bf16 = jnp.float32, jnp.bfloat16
    dma = pltpu.SemaphoreType.DMA
    cost, rho, vectors = pl.pallas_call(
        functools.partial(gw_kernel, mass_scale),
        out_shape=(
            jax.ShapeDtypeStruct((BLOCK, BLOCK), f32),
            jax.ShapeDtypeStruct((BLOCK, LANES), f32),
            jax.ShapeDtypeStruct((4 * TILES, LANES), f32),
        ),
        in_specs=[hbm, hbm, hbm, smem, smem],
        out_specs=(vmem, vmem, vmem),
        scratch_shapes=[
            pltpu.VMEM((PARTS, 32, BLOCK, WIDTH), bf16),
            pltpu.VMEM((PARTS, 4, BLOCK, WIDTH), bf16),
            pltpu.VMEM((PARTS, BLOCK, WIDTH), f32),
            pltpu.VMEM((32, BLOCK, BLOCK), bf16),
            pltpu.VMEM((4, BLOCK, BLOCK), bf16),
            pltpu.VMEM((BLOCK, BLOCK), f32),
            pltpu.VMEM((BLOCK, LANES), f32),
            pltpu.VMEM((SWEEPS, 4, TILES, LANES), f32),
            pltpu.VMEM((SWEEPS, 32, TILES, LANES), f32),
            dma((3,)),
            dma((PARTS,)),
            dma((PARTS, len(STEPS), 2, 2)),
            dma((PARTS, len(STEPS))),
            dma((PARTS,)),
            dma((PARTS, 6)),
            dma((SWEEPS,)),
            dma((SWEEPS,)),
            dma((SWEEPS,)),
            dma((SWEEPS,)),
        ],
        compiler_params=pltpu.CompilerParams(
            collective_id=0, has_side_effects=True, vmem_limit_bytes=56 * 1024 * 1024
        ),
        name="gw_step",
    )(graph_one, graph_two, coupling, sizes_one, sizes_two)
    plan, row_potential, col_potential = pl.pallas_call(
        functools.partial(finish_kernel, mass_scale),
        out_shape=(
            jax.ShapeDtypeStruct((BLOCK, BLOCK), f32),
            jax.ShapeDtypeStruct((TILES, LANES), f32),
            jax.ShapeDtypeStruct((TILES, LANES), f32),
        ),
        in_specs=[vmem, vmem, vmem],
        out_specs=(vmem, vmem, vmem),
        name="finish",
    )(cost, rho, vectors)
    return plan, row_potential.reshape(BLOCK), col_potential.reshape(BLOCK)


def solution(mesh):
    return jax.shard_map(
        body,
        mesh=mesh,
        in_specs=(P("row", None), P("col", None), P("row", "col"), P(), P()),
        out_specs=(P("row", "col"), P("row"), P("col")),
        check_vma=False,
    )
```

```python
import functools
import math

import jax
import jax.numpy as jnp
from jax import lax
from jax.experimental import pallas as pl
from jax.experimental.pallas import tpu as pltpu
from jax.sharding import PartitionSpec as P

BLOCK = 512
SWEEPS = 5
LANES = 128
TILES = BLOCK // LANES
CHUNK = 64
WIDTHS = (384, 128)
BEGINS = (0, 384)
PARTS = len(WIDTHS)
OFFSETS = (0, -1, 1, 2)
STEPS = tuple((first, second) for second in OFFSETS for first in OFFSETS)
HALF = BLOCK // 2
UNIT = BLOCK // 4
AFTER = ((1, 8, 40),)
LAG = 2
MESH = pl.DeviceIdType.MESH

very_low = -1e30


def plane_neighbours():
    steps = []
    for dx in range(4):
        for dz in range(4):
            for dc in range(2):
                if dx or dz or dc:
                    far = min(dx, 4 - dx) + min(dz, 4 - dz)
                    steps.append((-far, -dc, dx, dz, dc))
    return [step[2:] for step in sorted(steps)]


def diagonal():
    return lax.broadcasted_iota(jnp.int32, (LANES, LANES), 0) == lax.broadcasted_iota(
        jnp.int32, (LANES, LANES), 1
    )


COLUMN_US, HOP_US, SLOT_US, AHEAD_US = 1.405 / 256, 2.5, 1.0, 2.8


def sends_of(part, half, turn, first, second):
    onward = 1 if turn == 0 else -1
    out = []
    if second == 0:
        if first == 0:
            for way in (1, -1):
                out.append((0, way, (-way, 0), 4 if way == onward else 3))
        elif first == -onward:
            out.append((0, onward, (2, 0), 3))
        for way in (1, -1):
            out.append((1, way, (first, -way), 2 if way == onward else 1))
    elif second == -onward:
        out.append((1, onward, (first, 2), 1))
    return out


def timetable():
    arrival = {
        (part, half, turn, 0, 0): 0.0
        for part in range(PARTS)
        for half in range(2)
        for turn in range(2)
    }
    free = {(axis, way): 0.0 for axis in range(2) for way in (1, -1)}
    pending, known, slots, now = [], set(), [], 0.0
    while len(known) < PARTS * 4 * len(STEPS):
        fresh = sorted(
            (unit for unit in arrival if arrival[unit] <= now and unit not in known),
            key=lambda unit: (arrival[unit], unit),
        )
        known.update(fresh)
        for unit in fresh:
            pending += [(unit, *send) for send in sends_of(*unit)]
        sends = []
        for axis, way in free:
            while max(free[axis, way], now) - now < AHEAD_US:
                ready = [
                    send
                    for send in pending
                    if send[2] == way and (send[1] + send[0][1]) % 2 == axis
                ]
                if not ready:
                    break
                best = min(ready, key=lambda send: (send[0][0], -send[4]))
                pending.remove(best)
                free[axis, way] = (
                    max(free[axis, way], now) + COLUMN_US * WIDTHS[best[0][0]]
                )
                arrival[best[0][:3] + best[3]] = free[axis, way] + HOP_US
                sends.append(best)
        slots.append((fresh, sends))
        now += SLOT_US
    return slots


def group_of(unit):
    part, half, turn, first, second = unit
    if second == 2:
        return (part, first, second)
    if second and second != (-1 if turn == 0 else 1):
        return (part, turn, first, second)
    return unit


def grouped(slots):
    size, seen, out = {}, {}, []
    for fresh, _ in slots:
        for unit in fresh:
            size[group_of(unit)] = size.get(group_of(unit), 0) + 1
    for fresh, sends in slots:
        ready = []
        for unit in fresh:
            group = group_of(unit)
            seen.setdefault(group, []).append(unit)
            if len(seen[group]) == size[group]:
                ready.append((group, seen[group]))
        out.append((ready, sends))
    return out, {group: index for index, group in enumerate(size) if group[-2:] != (0, 0)}


def items_of(slots):
    count, work, last = {}, {}, -1
    for index, (ready, _) in enumerate(slots):
        for part, _, _, first, second in (unit for _, units in ready for unit in units):
            key = (part, STEPS.index((first, second)))
            count[key] = count.get(key, 0) + 1
            if count[key] == 4:
                pace = 2 if part == 0 else 1
                last = max(2 * (index + LAG), last + pace)
                work[last] = key
    return work


def plan_of_moves():
    return grouped(timetable())


def gw_kernel(
    mass_scale,
    graph_one_ref,
    graph_two_ref,
    coupling_ref,
    sizes_one_ref,
    sizes_two_ref,
    cost_ref,
    rho_ref,
    vectors_ref,
    *scratch,
):
    (
        plan_wide,
        plan_slim,
        first_wide,
        first_slim,
        total_wide,
        total_slim,
        one_ref,
        two_ref,
        loaded_ref,
        squares_ref,
        row_box,
        col_box,
        load_sem,
        one_sem,
        plan_send,
        plan_recv,
        pair_recv,
        first_send,
        first_recv,
        row_send,
        row_recv,
        col_send,
        col_recv,
    ) = scratch
    plans = [plan_wide, plan_slim]
    firsts = [first_wide, first_slim]
    totals = [total_wide, total_slim]
    load_coupling = pltpu.make_async_copy(coupling_ref, loaded_ref, load_sem.at[0])
    load_coupling.start()
    row = lax.axis_index("row")
    col = lax.axis_index("col")
    x, z, core = row // 8, (row // 2) % 4, row % 2
    other = 1 - core
    partner = row + 1 - 2 * core

    def around(value):
        return [value] + [
            jnp.where(value >= 4 - step, value + step - 4, value + step) for step in (1, 2, 3)
        ]

    xs, zs = [8 * value for value in around(x)], [2 * value for value in around(z)]
    _, up, across, down = around(col)
    row_peers = [across, up, down]
    col_peers = [
        xs[dx] + zs[dz] + (other if dc else core) for dx, dz, dc in plane_neighbours()
    ]
    places = [[xs[dx] + zs[dz] + core for dz in range(4)] for dx in range(4)]

    barrier = pltpu.get_barrier_semaphore()
    for peer in row_peers:
        pl.semaphore_signal(barrier, inc=1, device_id=(row, peer), device_id_type=MESH)
    for peer in col_peers:
        pl.semaphore_signal(barrier, inc=1, device_id=(peer, col), device_id_type=MESH)

    load_two = []
    for block in range(4):
        load_two.append(
            pltpu.make_async_copy(
                graph_two_ref.at[:, pl.ds(block * BLOCK, BLOCK)], two_ref.at[block], load_sem.at[1]
            )
        )
    total_one = jnp.float32(0)
    for block in range(sizes_one_ref.shape[0]):
        total_one = total_one + sizes_one_ref[block].astype(jnp.float32)
    total_two = jnp.float32(0)
    for block in range(sizes_two_ref.shape[0]):
        total_two = total_two + sizes_two_ref[block].astype(jnp.float32)
    all_one = jnp.full((TILES, LANES), total_one, jnp.float32)
    all_two = jnp.full((TILES, LANES), total_two, jnp.float32)
    log_one = jnp.log2(all_one)
    log_two = jnp.log2(all_two)
    size_one = sizes_one_ref[row]
    size_two = sizes_two_ref[col]
    slot = lax.broadcasted_iota(jnp.int32, (TILES, LANES), 0) * LANES + lax.broadcasted_iota(
        jnp.int32, (TILES, LANES), 1
    )
    live_row = slot < size_one
    live_col = slot < size_two
    diag = diagonal()

    def live_part(start, width, offset=0):
        ids = lax.broadcasted_iota(jnp.int32, (CHUNK, width), 0) + start
        lanes = lax.broadcasted_iota(jnp.int32, (CHUNK, width), 1) + offset
        return (ids < size_one) & (lanes < size_two)

    load_coupling.wait()
    for start in range(0, BLOCK, CHUNK):
        rows = pl.ds(start, CHUNK)
        for part in range(PARTS):
            kept = jnp.where(
                live_part(start, WIDTHS[part], BEGINS[part]),
                loaded_ref[rows, pl.ds(BEGINS[part], WIDTHS[part])],
                0.0,
            )
            plans[part][row, rows, :] = kept.astype(jnp.bfloat16)
    squares_ref[...] = jnp.zeros_like(squares_ref)
    pl.semaphore_wait(barrier, 34)

    def place(half, first, second):
        dx, dz = (first, second) if half == 0 else (second, first)
        return places[dx % 4][dz % 4]

    def wait_bytes(ref, sem):
        pltpu.make_async_copy(ref, ref, sem).wait()

    def piece_of(part, half, turn, first, second):
        rows = pl.ds(half * HALF + turn * UNIT, UNIT)
        return plans[part].at[place(half, first, second), rows, :]

    def moves(ready, sends, fetched):
        for group, units in ready:
            if group in semaphores:
                rows = pl.ds(0, UNIT * len(units))
                wait_bytes(plans[group[0]].at[0, rows, :], plan_recv.at[semaphores[group]])
        for unit, axis, way, seen, _ in sends:
            part, half, turn, first, second = unit
            piece = piece_of(*unit)
            target = place(half, way, 0) if axis == 0 else place(half, 0, way)
            pltpu.make_async_remote_copy(
                src_ref=piece,
                dst_ref=piece,
                send_sem=plan_send.at[part],
                recv_sem=plan_recv.at[semaphores[group_of((part, half, turn, *seen))]],
                device_id=(target, col),
                device_id_type=MESH,
            ).start()
        for unit in (unit for _, units in ready for unit in units):
            part, half, turn, first, second = unit
            piece = piece_of(*unit)
            pltpu.make_async_remote_copy(
                src_ref=piece,
                dst_ref=piece,
                send_sem=plan_send.at[part],
                recv_sem=pair_recv.at[part, STEPS.index((first, second))],
                device_id=(partner, col),
                device_id_type=MESH,
            ).start()
        for step in fetched:
            for half in range(2):
                for owner in (core, other):
                    source = place(half, *STEPS[step]) - core + owner
                    start = pl.multiple_of(source * BLOCK + half * HALF, HALF)
                    pltpu.make_async_copy(
                        graph_one_ref.at[:, pl.ds(start, HALF)],
                        one_ref.at[source, :, pl.ds(half * HALF, HALF)],
                        one_sem.at[step],
                    ).start()

    def pick(options, index):
        value = options[OFFSETS[-1] % 4]
        for place_of, offset in enumerate(OFFSETS[:-1]):
            value = jnp.where(index == place_of, options[offset % 4], value)
        return value

    def multiply(code):
        part = jnp.where(code >= len(STEPS), 1, 0)
        step = code - len(STEPS) * part
        second = (
            jnp.where(step >= 4, 1, 0) + jnp.where(step >= 8, 1, 0) + jnp.where(step >= 12, 1, 0)
        )
        first = step - 4 * second
        chips = (pick(xs, first) + pick(zs, second), pick(xs, second) + pick(zs, first))

        def add_products(plan, total_ref):
            for start in range(0, BLOCK, HALF):
                total = total_ref[pl.ds(start, HALF), :]
                for half in range(2):
                    rows = pl.ds(half * HALF, HALF)
                    for owner in (core, other):
                        source = chips[half] + owner
                        total = total + jnp.dot(
                            one_ref[source, pl.ds(start, HALF), rows],
                            plan[source, rows, :],
                            preferred_element_type=jnp.float32,
                        )
                total_ref[pl.ds(start, HALF), :] = total

        @pl.when(part > 0)
        def _():
            wait_bytes(plan_slim.at[0], pair_recv.at[part, step])
            add_products(plan_slim, total_slim)

        @pl.when(part == 0)
        def _():
            wait_bytes(plan_wide.at[0], pair_recv.at[part, step])
            wait_bytes(one_ref.at[pl.ds(0, 2)], one_sem.at[step])
            add_products(plan_wide, total_wide)
            for start in range(0, BLOCK, CHUNK):
                squares = squares_ref[pl.ds(start, CHUNK), :]
                for half in range(2):
                    for owner in (core, other):
                        source = chips[half] + owner
                        size = sizes_one_ref[source]
                        for tile in range(2):
                            lanes = half * HALF + tile * LANES
                            ids = lax.broadcasted_iota(jnp.int32, (CHUNK, LANES), 1) + lanes
                            value = one_ref[
                                source, pl.ds(start, CHUNK), pl.ds(lanes, LANES)
                            ].astype(jnp.float32)
                            squares = squares + jnp.where(ids < size, value * value, 0.0)
                squares_ref[pl.ds(start, CHUNK), :] = squares

    def first_copy(part, half, source, key, target):
        piece = firsts[part].at[source, pl.ds(half * HALF, HALF), :]
        return pltpu.make_async_remote_copy(
            src_ref=piece,
            dst_ref=piece,
            send_sem=first_send.at[part],
            recv_sem=first_recv.at[part, key],
            device_id=(row, target),
            device_id_type=MESH,
        )

    def first_start(part):
        for start in range(0, BLOCK, CHUNK):
            rows = pl.ds(start, CHUNK)
            firsts[part][col, rows, :] = totals[part][rows, :].astype(jnp.bfloat16)
        first_copy(part, 0, col, 0, up).start()
        first_copy(part, 1, col, 1, down).start()
        first_copy(part, 1, col, 2, up).start()
        first_copy(part, 0, col, 3, down).start()

    def first_wait(part, half, source, key):
        wait_bytes(firsts[part].at[source, pl.ds(half * HALF, HALF), :], first_recv.at[part, key])

    def first_onward(part):
        first_wait(part, 0, down, 0)
        first_copy(part, 0, down, 4, up).start()
        first_wait(part, 1, up, 1)
        first_copy(part, 1, up, 5, down).start()

    def cross_add(part, source, fresh=False):
        added = lax.dot_general(
            firsts[part][source],
            two_ref[source, :, pl.ds(BEGINS[part], WIDTHS[part])],
            (((1,), (1,)), ((), ())),
            preferred_element_type=jnp.float32,
        )
        if fresh:
            cost_ref[...] = added
        else:
            cost_ref[...] += added

    def first_end(part):
        cross_add(part, col, fresh=part == 0)
        first_wait(part, 1, down, 2)
        cross_add(part, down)
        first_wait(part, 0, up, 3)
        cross_add(part, up)
        first_wait(part, 0, across, 4)
        first_wait(part, 1, across, 5)
        cross_add(part, across)

    slots, semaphores = plan_of_moves()
    work = items_of(slots)
    length = max(work) // 2 + 1
    slots = slots + [([], [])] * (length - len(slots))
    order = [work[turn][1] for turn in sorted(work) if work[turn][0] == 0]
    fetches = [order[:4]] + [[step] for step in order[4:]] + [[]] * length
    whole = [max(turn // 2 for turn in work if work[turn][0] == part) for part in range(PARTS)]
    extra = {}
    for part in range(PARTS - 1):
        for after, run in zip(AFTER[part], (first_start, first_onward, first_end)):
            extra.setdefault(min(whole[part] + after, length), []).append(
                functools.partial(run, part)
            )
    for total in totals:
        total[...] = jnp.zeros_like(total)
    moves(*slots[0], fetches[0])
    for copy in load_two:
        copy.start()
    wait_bytes(two_ref, load_sem.at[1])
    col_square = []
    for tile in range(TILES):
        summed = []
        for start in range(tile * LANES, (tile + 1) * LANES, CHUNK):
            gathered = jnp.zeros((CHUNK, LANES), jnp.float32)
            for block in range(4):
                for lane in range(TILES):
                    ids = lax.broadcasted_iota(jnp.int32, (CHUNK, LANES), 1) + lane * LANES
                    value = two_ref[block, pl.ds(start, CHUNK), pl.ds(lane * LANES, LANES)].astype(
                        jnp.float32
                    )
                    gathered = gathered + jnp.where(
                        ids < sizes_two_ref[block], value * value, 0.0
                    )
            summed.append(
                jnp.broadcast_to(jnp.sum(gathered, axis=1, keepdims=True), (CHUNK, LANES))
            )
        vectors_ref[pl.ds(12 + tile, 1), :] = jnp.sum(
            jnp.where(diag, jnp.concatenate(summed, axis=0), 0.0), axis=0, keepdims=True
        )

    def one_slot(slot, carry):
        for group in range(0, length, 8):

            @pl.when((slot >= group) & (slot < group + 8))
            def _():
                for index in range(max(group, 1), min(group + 8, length)):
                    if slots[index] != ([], []) or fetches[index] or index in extra:

                        @pl.when(slot == index)
                        def _():
                            moves(*slots[index], fetches[index])
                            for run in extra.get(index, ()):
                                run()

        def one_turn(turn, carry):
            code = jnp.int32(-1)
            for index, (part, step) in work.items():
                code = jnp.where(2 * slot + turn == index, part * len(STEPS) + step, code)

            @pl.when(code >= 0)
            def _():
                multiply(code)

            return carry

        return lax.fori_loop(0, 2, one_turn, carry)

    lax.fori_loop(0, length, one_slot, 0)
    first_start(PARTS - 1)
    for run in extra.get(length, ()):
        run()
    for tile in range(TILES):
        column = jnp.broadcast_to(
            jnp.sum(squares_ref[pl.ds(tile * LANES, LANES), :], axis=1, keepdims=True),
            (LANES, LANES),
        )
        vectors_ref[pl.ds(8 + tile, 1), :] = jnp.sum(
            jnp.where(diag, column, 0.0), axis=0, keepdims=True
        )
    first_onward(PARTS - 1)
    first_end(PARTS - 1)

    scale = jnp.float32(2.0 / math.sqrt(mass_scale) * math.log2(math.e))
    for start in range(0, BLOCK, CHUNK):
        rows = pl.ds(start, CHUNK)
        cost_ref[rows, :] = jnp.where(
            live_part(start, BLOCK), cost_ref[rows, :] * scale, jnp.float32(very_low)
        )

    def exchange(box, mine, sweep, send, recv, targets):
        for target in targets:
            pltpu.make_async_remote_copy(
                src_ref=box.at[sweep, mine],
                dst_ref=box.at[sweep, mine],
                send_sem=send.at[0],
                recv_sem=recv.at[sweep],
                device_id=target,
                device_id_type=MESH,
            ).start()
        wait_bytes(box.at[sweep, pl.ds(0, len(targets))], recv.at[sweep])
        logs = box[sweep]
        top = jnp.max(logs, axis=0)
        return top + jnp.log2(jnp.sum(jnp.exp2(logs - top[None]), axis=0))

    def gamma_row(gamma):
        return jnp.concatenate([gamma[t : t + 1, :] for t in range(TILES)], axis=1)

    def sweep_body(sweep, gamma):
        for tile in range(TILES):
            column = []
            for start in range(tile * LANES, (tile + 1) * LANES, CHUNK):
                values = cost_ref[pl.ds(start, CHUNK), :] + gamma_row(gamma)
                top = jnp.max(values, axis=1, keepdims=True)
                summed = jnp.sum(jnp.exp2(values - top), axis=1, keepdims=True)
                column.append(jnp.broadcast_to(top + jnp.log2(summed), (CHUNK, LANES)))
            column = jnp.concatenate(column, axis=0)
            row_box[sweep, col, pl.ds(tile, 1), :] = jnp.sum(
                jnp.where(diag, column, 0.0), axis=0, keepdims=True
            )
        lse = exchange(
            row_box, col, sweep, row_send, row_recv, [(row, peer) for peer in row_peers]
        )
        rho = jnp.where(live_row, -log_one - lse, 0.0)
        vectors_ref[pl.ds(0, TILES), :] = rho
        for tile in range(TILES):
            spread = jnp.broadcast_to(rho[tile : tile + 1, :], (LANES, LANES))
            rho_ref[pl.ds(tile * LANES, LANES), :] = jnp.broadcast_to(
                jnp.sum(jnp.where(diag, spread, 0.0), axis=1, keepdims=True), (LANES, LANES)
            )
        for tile in range(TILES):
            lanes = pl.ds(tile * LANES, LANES)
            tops, sums = [], []
            for start in range(0, BLOCK, 2 * CHUNK):
                rows = pl.ds(start, 2 * CHUNK)
                values = (cost_ref[rows, lanes] + rho_ref[rows, :]).reshape(
                    2 * CHUNK // 8, 8, LANES
                )
                top = jnp.max(values, axis=0)
                tops.append(top)
                sums.append(jnp.sum(jnp.exp2(values - top[None]), axis=0))
            high = functools.reduce(jnp.maximum, tops)
            high = jnp.max(high, axis=0, keepdims=True)
            summed = sum(s * jnp.exp2(t - high) for s, t in zip(sums, tops))
            col_box[sweep, row, pl.ds(tile, 1), :] = high + jnp.log2(
                jnp.sum(summed, axis=0, keepdims=True)
            )
        lse = exchange(
            col_box, row, sweep, col_send, col_recv, [(peer, col) for peer in col_peers]
        )
        return jnp.where(live_col, -log_two - lse, 0.0)

    gamma = lax.fori_loop(0, SWEEPS, sweep_body, jnp.zeros((TILES, LANES), jnp.float32))

    unit = jnp.float32(math.log(2.0) / math.sqrt(mass_scale))
    rho = vectors_ref[pl.ds(0, TILES), :]
    row_const = vectors_ref[pl.ds(8, TILES), :] / all_one
    col_const = vectors_ref[pl.ds(12, TILES), :] / all_two
    vectors_ref[pl.ds(4, TILES), :] = gamma
    vectors_ref[pl.ds(8, TILES), :] = jnp.where(live_row, rho * unit + row_const, 0.0)
    vectors_ref[pl.ds(12, TILES), :] = jnp.where(live_col, gamma * unit + col_const, 0.0)

    wait_bytes(row_box.at[:, pl.ds(0, 3)], row_send.at[0])
    wait_bytes(col_box.at[:, pl.ds(0, 31)], col_send.at[0])
    for part in range(PARTS):
        wait_bytes(plans[part].at[pl.ds(0, 31)], plan_send.at[part])
        wait_bytes(firsts[part].at[pl.ds(0, 3)], first_send.at[part])


def finish_kernel(mass_scale, cost_ref, rho_ref, vectors_ref, plan_ref, row_ref, col_ref):
    gamma = jnp.concatenate([vectors_ref[pl.ds(4 + t, 1), :] for t in range(TILES)], axis=1)
    for start in range(0, BLOCK, CHUNK):
        rows = pl.ds(start, CHUNK)
        exponent = (
            cost_ref[rows, :] + jnp.concatenate([rho_ref[rows, :]] * TILES, axis=1) + gamma
        )
        plan_ref[rows, :] = jnp.float32(mass_scale) * jnp.exp2(exponent)
    row_ref[...] = vectors_ref[pl.ds(8, TILES), :]
    col_ref[...] = vectors_ref[pl.ds(12, TILES), :]


def body(graph_one, graph_two, coupling, sizes_one, sizes_two):
    graph_one, graph_two, coupling, sizes_one, sizes_two = (
        pltpu.with_memory_space_constraint(value, pltpu.HBM)
        for value in (graph_one, graph_two, coupling, sizes_one, sizes_two)
    )
    mass_scale = float(graph_one.shape[1] * graph_two.shape[1])
    vmem = pl.BlockSpec(memory_space=pltpu.VMEM)
    smem = pl.BlockSpec(memory_space=pltpu.SMEM)
    hbm = pl.BlockSpec(memory_space=pltpu.HBM)
    f32, bf16 = jnp.float32, jnp.bfloat16
    dma = pltpu.SemaphoreType.DMA
    cost, rho, vectors = pl.pallas_call(
        functools.partial(gw_kernel, mass_scale),
        out_shape=(
            jax.ShapeDtypeStruct((BLOCK, BLOCK), f32),
            jax.ShapeDtypeStruct((BLOCK, LANES), f32),
            jax.ShapeDtypeStruct((4 * TILES, LANES), f32),
        ),
        in_specs=[hbm, hbm, hbm, smem, smem],
        out_specs=(vmem, vmem, vmem),
        scratch_shapes=[
            pltpu.VMEM((32, BLOCK, WIDTHS[0]), bf16),
            pltpu.VMEM((32, BLOCK, WIDTHS[1]), bf16),
            pltpu.VMEM((4, BLOCK, WIDTHS[0]), bf16),
            pltpu.VMEM((4, BLOCK, WIDTHS[1]), bf16),
            pltpu.VMEM((BLOCK, WIDTHS[0]), f32),
            pltpu.VMEM((BLOCK, WIDTHS[1]), f32),
            pltpu.VMEM((32, BLOCK, BLOCK), bf16),
            pltpu.VMEM((4, BLOCK, BLOCK), bf16),
            pltpu.VMEM((BLOCK, BLOCK), f32),
            pltpu.VMEM((BLOCK, LANES), f32),
            pltpu.VMEM((SWEEPS, 4, TILES, LANES), f32),
            pltpu.VMEM((SWEEPS, 32, TILES, LANES), f32),
            dma((2,)),
            dma((len(STEPS),)),
            dma((PARTS,)),
            dma((len(plan_of_moves()[1]) + 4 * PARTS,)),
            dma((PARTS, len(STEPS))),
            dma((PARTS,)),
            dma((PARTS, 6)),
            dma((1,)),
            dma((SWEEPS,)),
            dma((1,)),
            dma((SWEEPS,)),
        ],
        compiler_params=pltpu.CompilerParams(
            collective_id=0, has_side_effects=True, vmem_limit_bytes=52000 * 1024
        ),
        name="gw_step",
    )(graph_one, graph_two, coupling, sizes_one, sizes_two)
    plan, row_potential, col_potential = pl.pallas_call(
        functools.partial(finish_kernel, mass_scale),
        out_shape=(
            jax.ShapeDtypeStruct((BLOCK, BLOCK), f32),
            jax.ShapeDtypeStruct((TILES, LANES), f32),
            jax.ShapeDtypeStruct((TILES, LANES), f32),
        ),
        in_specs=[vmem, vmem, vmem],
        out_specs=(vmem, vmem, vmem),
        compiler_params=pltpu.CompilerParams(vmem_limit_bytes=8 * 1024 * 1024),
        name="finish",
    )(cost, rho, vectors)
    return plan, row_potential.reshape(BLOCK), col_potential.reshape(BLOCK)


def solution(mesh):
    return jax.shard_map(
        body,
        mesh=mesh,
        in_specs=(P("row", None), P("col", None), P("row", "col"), P(), P()),
        out_specs=(P("row", "col"), P("row"), P("col")),
        check_vma=False,
    )
```

```python
import functools
import math

import jax
import jax.numpy as jnp
from jax import lax
from jax.experimental import pallas as pl
from jax.experimental.pallas import tpu as pltpu
from jax.sharding import PartitionSpec as P

BLOCK = 512
SWEEPS = 5
LANES = 128
TILES = BLOCK // LANES
CHUNK = 64
WIDTHS = (384, 128)
BEGINS = (0, 384)
PARTS = len(WIDTHS)
OFFSETS = (0, -1, 1, 2)
STEPS = tuple((first, second) for second in OFFSETS for first in OFFSETS)
HALF = BLOCK // 2
UNIT = BLOCK // 4
AFTER = ((1, 8, 40),)
LAG = 2
MESH = pl.DeviceIdType.MESH

very_low = -1e30


def plane_neighbours():
    steps = []
    for dx in range(4):
        for dz in range(4):
            for dc in range(2):
                if dx or dz or dc:
                    far = min(dx, 4 - dx) + min(dz, 4 - dz)
                    steps.append((-far, -dc, dx, dz, dc))
    return [step[2:] for step in sorted(steps)]


def diagonal():
    return lax.broadcasted_iota(jnp.int32, (LANES, LANES), 0) == lax.broadcasted_iota(
        jnp.int32, (LANES, LANES), 1
    )


COLUMN_US, HOP_US, SLOT_US, AHEAD_US = 1.405 / 256, 2.5, 1.0, 2.8


def sends_of(part, half, turn, first, second):
    onward = 1 if turn == 0 else -1
    out = []
    if second == 0:
        if first == 0:
            for way in (1, -1):
                out.append((0, way, (-way, 0), 4 if way == onward else 3))
        elif first == -onward:
            out.append((0, onward, (2, 0), 3))
        for way in (1, -1):
            out.append((1, way, (first, -way), 2 if way == onward else 1))
    elif second == -onward:
        out.append((1, onward, (first, 2), 1))
    return out


def timetable():
    arrival = {
        (part, half, turn, 0, 0): 0.0
        for part in range(PARTS)
        for half in range(2)
        for turn in range(2)
    }
    free = {(axis, way): 0.0 for axis in range(2) for way in (1, -1)}
    pending, known, slots, now = [], set(), [], 0.0
    while len(known) < PARTS * 4 * len(STEPS):
        fresh = sorted(
            (unit for unit in arrival if arrival[unit] <= now and unit not in known),
            key=lambda unit: (arrival[unit], unit),
        )
        known.update(fresh)
        for unit in fresh:
            pending += [(unit, *send) for send in sends_of(*unit)]
        sends = []
        for axis, way in free:
            while max(free[axis, way], now) - now < AHEAD_US:
                ready = [
                    send
                    for send in pending
                    if send[2] == way and (send[1] + send[0][1]) % 2 == axis
                ]
                if not ready:
                    break
                best = min(ready, key=lambda send: (send[0][0], -send[4]))
                pending.remove(best)
                free[axis, way] = (
                    max(free[axis, way], now) + COLUMN_US * WIDTHS[best[0][0]]
                )
                arrival[best[0][:3] + best[3]] = free[axis, way] + HOP_US
                sends.append(best)
        slots.append((fresh, sends))
        now += SLOT_US
    return slots


def group_of(unit):
    part, half, turn, first, second = unit
    if second == 2:
        return (part, first, second)
    if second and second != (-1 if turn == 0 else 1):
        return (part, turn, first, second)
    return unit


def grouped(slots):
    size, seen, out = {}, {}, []
    for fresh, _ in slots:
        for unit in fresh:
            size[group_of(unit)] = size.get(group_of(unit), 0) + 1
    for fresh, sends in slots:
        ready = []
        for unit in fresh:
            group = group_of(unit)
            seen.setdefault(group, []).append(unit)
            if len(seen[group]) == size[group]:
                ready.append((group, seen[group]))
        out.append((ready, sends))
    groups = [group for group in size if group[-2:] != (0, 0)]
    return out, {group: index for index, group in enumerate(groups)}


def items_of(slots):
    count, work, last = {}, {}, -1
    for index, (ready, _) in enumerate(slots):
        for part, _, _, first, second in (unit for _, units in ready for unit in units):
            key = (part, STEPS.index((first, second)))
            count[key] = count.get(key, 0) + 1
            if count[key] == 4:
                pace = 2 if part == 0 else 1
                last = max(2 * (index + LAG), last + pace)
                work[last] = key
    return work


def plan_of_moves():
    return grouped(timetable())


def gw_kernel(
    mass_scale,
    graph_one_ref,
    graph_two_ref,
    coupling_ref,
    sizes_one_ref,
    sizes_two_ref,
    cost_ref,
    rho_ref,
    vectors_ref,
    *scratch,
):
    (
        plan_wide,
        plan_slim,
        first_wide,
        first_slim,
        total_wide,
        total_slim,
        one_ref,
        two_ref,
        loaded_ref,
        squares_ref,
        row_box,
        col_box,
        load_sem,
        one_sem,
        plan_send,
        plan_recv,
        pair_recv,
        first_send,
        first_recv,
        row_send,
        row_recv,
        col_send,
        col_recv,
    ) = scratch
    plans = [plan_wide, plan_slim]
    firsts = [first_wide, first_slim]
    totals = [total_wide, total_slim]
    load_coupling = pltpu.make_async_copy(coupling_ref, loaded_ref, load_sem.at[0])
    load_coupling.start()
    row = lax.axis_index("row")
    col = lax.axis_index("col")
    x, z, core = row // 8, (row // 2) % 4, row % 2
    other = 1 - core
    partner = row + 1 - 2 * core

    def around(value):
        return [value] + [
            jnp.where(value >= 4 - step, value + step - 4, value + step) for step in (1, 2, 3)
        ]

    xs, zs = [8 * value for value in around(x)], [2 * value for value in around(z)]
    _, up, across, down = around(col)
    row_peers = [across, up, down]
    col_peers = [
        xs[dx] + zs[dz] + (other if dc else core) for dx, dz, dc in plane_neighbours()
    ]
    places = [[xs[dx] + zs[dz] + core for dz in range(4)] for dx in range(4)]

    barrier = pltpu.get_barrier_semaphore()
    for peer in (up, down):
        pl.semaphore_signal(barrier, inc=1, device_id=(row, peer), device_id_type=MESH)
    for peer in (places[1][0], places[3][0], places[0][1], places[0][3], partner):
        pl.semaphore_signal(barrier, inc=1, device_id=(peer, col), device_id_type=MESH)

    load_two = []
    for block in range(4):
        load_two.append(
            pltpu.make_async_copy(
                graph_two_ref.at[:, pl.ds(block * BLOCK, BLOCK)], two_ref.at[block], load_sem.at[1]
            )
        )
    total_one = jnp.float32(0)
    for block in range(sizes_one_ref.shape[0]):
        total_one = total_one + sizes_one_ref[block].astype(jnp.float32)
    total_two = jnp.float32(0)
    for block in range(sizes_two_ref.shape[0]):
        total_two = total_two + sizes_two_ref[block].astype(jnp.float32)
    all_one = jnp.full((TILES, LANES), total_one, jnp.float32)
    all_two = jnp.full((TILES, LANES), total_two, jnp.float32)
    log_one = jnp.log2(all_one)
    log_two = jnp.log2(all_two)
    size_one = sizes_one_ref[row]
    size_two = sizes_two_ref[col]
    slot = lax.broadcasted_iota(jnp.int32, (TILES, LANES), 0) * LANES + lax.broadcasted_iota(
        jnp.int32, (TILES, LANES), 1
    )
    live_row = slot < size_one
    live_col = slot < size_two
    diag = diagonal()

    def live_part(start, width, offset=0):
        ids = lax.broadcasted_iota(jnp.int32, (CHUNK, width), 0) + start
        lanes = lax.broadcasted_iota(jnp.int32, (CHUNK, width), 1) + offset
        return (ids < size_one) & (lanes < size_two)

    load_coupling.wait()
    for start in range(0, BLOCK, CHUNK):
        rows = pl.ds(start, CHUNK)
        for part in range(PARTS):
            kept = jnp.where(
                live_part(start, WIDTHS[part], BEGINS[part]),
                loaded_ref[rows, pl.ds(BEGINS[part], WIDTHS[part])],
                0.0,
            )
            plans[part][row, rows, :] = kept.astype(jnp.bfloat16)
    squares_ref[...] = jnp.zeros_like(squares_ref)
    pl.semaphore_wait(barrier, 7)

    def place(half, first, second):
        dx, dz = (first, second) if half == 0 else (second, first)
        return places[dx % 4][dz % 4]

    def wait_bytes(ref, sem):
        pltpu.make_async_copy(ref, ref, sem).wait()

    def piece_of(part, half, turn, first, second):
        rows = pl.ds(half * HALF + turn * UNIT, UNIT)
        return plans[part].at[place(half, first, second), rows, :]

    def moves(ready, sends, fetched):
        for group, units in ready:
            if group in semaphores:
                rows = pl.ds(0, UNIT * len(units))
                wait_bytes(plans[group[0]].at[0, rows, :], plan_recv.at[semaphores[group]])
        for unit, axis, way, seen, _ in sends:
            part, half, turn, first, second = unit
            piece = piece_of(*unit)
            target = place(half, way, 0) if axis == 0 else place(half, 0, way)
            pltpu.make_async_remote_copy(
                src_ref=piece,
                dst_ref=piece,
                send_sem=plan_send.at[part],
                recv_sem=plan_recv.at[semaphores[group_of((part, half, turn, *seen))]],
                device_id=(target, col),
                device_id_type=MESH,
            ).start()
        for unit in (unit for _, units in ready for unit in units):
            part, half, turn, first, second = unit
            piece = piece_of(*unit)
            pltpu.make_async_remote_copy(
                src_ref=piece,
                dst_ref=piece,
                send_sem=plan_send.at[part],
                recv_sem=pair_recv.at[part, STEPS.index((first, second))],
                device_id=(partner, col),
                device_id_type=MESH,
            ).start()
        for step in fetched:
            for half in range(2):
                for owner in (core, other):
                    source = place(half, *STEPS[step]) - core + owner
                    start = pl.multiple_of(source * BLOCK + half * HALF, HALF)
                    pltpu.make_async_copy(
                        graph_one_ref.at[:, pl.ds(start, HALF)],
                        one_ref.at[source, :, pl.ds(half * HALF, HALF)],
                        one_sem.at[step],
                    ).start()

    def pick(options, index):
        value = options[OFFSETS[-1] % 4]
        for place_of, offset in enumerate(OFFSETS[:-1]):
            value = jnp.where(index == place_of, options[offset % 4], value)
        return value

    def multiply(code):
        part = jnp.where(code >= len(STEPS), 1, 0)
        step = code - len(STEPS) * part
        second = (
            jnp.where(step >= 4, 1, 0) + jnp.where(step >= 8, 1, 0) + jnp.where(step >= 12, 1, 0)
        )
        first = step - 4 * second
        chips = (pick(xs, first) + pick(zs, second), pick(xs, second) + pick(zs, first))

        def add_products(plan, total_ref):
            for start in range(0, BLOCK, HALF):
                total = total_ref[pl.ds(start, HALF), :]
                for half in range(2):
                    rows = pl.ds(half * HALF, HALF)
                    for owner in (core, other):
                        source = chips[half] + owner
                        total = total + jnp.dot(
                            one_ref[source, pl.ds(start, HALF), rows],
                            plan[source, rows, :],
                            preferred_element_type=jnp.float32,
                        )
                total_ref[pl.ds(start, HALF), :] = total

        @pl.when(part > 0)
        def _():
            wait_bytes(plan_slim.at[0], pair_recv.at[part, step])
            add_products(plan_slim, total_slim)

        @pl.when(part == 0)
        def _():
            wait_bytes(plan_wide.at[0], pair_recv.at[part, step])
            wait_bytes(one_ref.at[pl.ds(0, 2)], one_sem.at[step])
            add_products(plan_wide, total_wide)
            for start in range(0, BLOCK, CHUNK):
                squares = squares_ref[pl.ds(start, CHUNK), :]
                for half in range(2):
                    for owner in (core, other):
                        source = chips[half] + owner
                        size = sizes_one_ref[source]
                        for tile in range(2):
                            lanes = half * HALF + tile * LANES
                            ids = lax.broadcasted_iota(jnp.int32, (CHUNK, LANES), 1) + lanes
                            value = one_ref[
                                source, pl.ds(start, CHUNK), pl.ds(lanes, LANES)
                            ].astype(jnp.float32)
                            squares = squares + jnp.where(ids < size, value * value, 0.0)
                squares_ref[pl.ds(start, CHUNK), :] = squares

    def first_copy(part, half, source, key, target):
        piece = firsts[part].at[source, pl.ds(half * HALF, HALF), :]
        return pltpu.make_async_remote_copy(
            src_ref=piece,
            dst_ref=piece,
            send_sem=first_send.at[part],
            recv_sem=first_recv.at[part, key],
            device_id=(row, target),
            device_id_type=MESH,
        )

    def first_start(part):
        for start in range(0, BLOCK, CHUNK):
            rows = pl.ds(start, CHUNK)
            firsts[part][col, rows, :] = totals[part][rows, :].astype(jnp.bfloat16)
        first_copy(part, 0, col, 0, up).start()
        first_copy(part, 1, col, 1, down).start()
        first_copy(part, 1, col, 2, up).start()
        first_copy(part, 0, col, 3, down).start()

    def first_wait(part, half, source, key):
        wait_bytes(firsts[part].at[source, pl.ds(half * HALF, HALF), :], first_recv.at[part, key])

    def first_onward(part):
        first_wait(part, 0, down, 0)
        first_copy(part, 0, down, 4, up).start()
        first_wait(part, 1, up, 1)
        first_copy(part, 1, up, 5, down).start()

    def cross_add(part, source, fresh=False):
        added = lax.dot_general(
            firsts[part][source],
            two_ref[source, :, pl.ds(BEGINS[part], WIDTHS[part])],
            (((1,), (1,)), ((), ())),
            preferred_element_type=jnp.float32,
        )
        if fresh:
            cost_ref[...] = added
        else:
            cost_ref[...] += added

    def first_end(part):
        cross_add(part, col, fresh=part == 0)
        first_wait(part, 1, down, 2)
        cross_add(part, down)
        first_wait(part, 0, up, 3)
        cross_add(part, up)
        first_wait(part, 0, across, 4)
        first_wait(part, 1, across, 5)
        cross_add(part, across)

    def square_columns():
        wait_bytes(two_ref, load_sem.at[1])
        col_square = []
        for tile in range(TILES):
            summed = []
            for start in range(tile * LANES, (tile + 1) * LANES, CHUNK):
                gathered = jnp.zeros((CHUNK, LANES), jnp.float32)
                for block in range(4):
                    for lane in range(TILES):
                        ids = lax.broadcasted_iota(jnp.int32, (CHUNK, LANES), 1) + lane * LANES
                        value = two_ref[block, pl.ds(start, CHUNK), pl.ds(lane * LANES, LANES)].astype(
                            jnp.float32
                        )
                        gathered = gathered + jnp.where(
                            ids < sizes_two_ref[block], value * value, 0.0
                        )
                summed.append(
                    jnp.broadcast_to(jnp.sum(gathered, axis=1, keepdims=True), (CHUNK, LANES))
                )
            vectors_ref[pl.ds(12 + tile, 1), :] = jnp.sum(
                jnp.where(diag, jnp.concatenate(summed, axis=0), 0.0), axis=0, keepdims=True
            )

    slots, semaphores = plan_of_moves()
    work = items_of(slots)
    length = max(work) // 2 + 1
    slots = slots + [([], [])] * (length - len(slots))
    order = [work[turn][1] for turn in sorted(work) if work[turn][0] == 0]
    fetches = [order[:4]] + [[step] for step in order[4:]] + [[]] * length
    whole = [max(turn // 2 for turn in work if work[turn][0] == part) for part in range(PARTS)]
    extra = {5: [square_columns]}
    for part in range(PARTS - 1):
        for after, run in zip(AFTER[part], (first_start, first_onward, first_end)):
            extra.setdefault(min(whole[part] + after, length), []).append(
                functools.partial(run, part)
            )
    for total in totals:
        total[...] = jnp.zeros_like(total)
    moves(*slots[0], fetches[0])
    for copy in load_two:
        copy.start()
    def one_slot(slot, carry):
        for group in range(0, length, 8):

            @pl.when((slot >= group) & (slot < group + 8))
            def _():
                for index in range(max(group, 1), min(group + 8, length)):
                    if slots[index] != ([], []) or fetches[index] or index in extra:

                        @pl.when(slot == index)
                        def _():
                            moves(*slots[index], fetches[index])
                            for run in extra.get(index, ()):
                                run()

        def one_turn(turn, carry):
            code = jnp.int32(-1)
            for index, (part, step) in work.items():
                code = jnp.where(2 * slot + turn == index, part * len(STEPS) + step, code)

            @pl.when(code >= 0)
            def _():
                multiply(code)

            return carry

        return lax.fori_loop(0, 2, one_turn, carry)

    lax.fori_loop(0, length, one_slot, 0)
    first_start(PARTS - 1)
    for run in extra.get(length, ()):
        run()
    for tile in range(TILES):
        column = jnp.broadcast_to(
            jnp.sum(squares_ref[pl.ds(tile * LANES, LANES), :], axis=1, keepdims=True),
            (LANES, LANES),
        )
        vectors_ref[pl.ds(8 + tile, 1), :] = jnp.sum(
            jnp.where(diag, column, 0.0), axis=0, keepdims=True
        )
    first_onward(PARTS - 1)
    first_end(PARTS - 1)

    scale = jnp.float32(2.0 / math.sqrt(mass_scale) * math.log2(math.e))
    for start in range(0, BLOCK, CHUNK):
        rows = pl.ds(start, CHUNK)
        cost_ref[rows, :] = jnp.where(
            live_part(start, BLOCK), cost_ref[rows, :] * scale, jnp.float32(very_low)
        )

    def exchange(box, mine, sweep, send, recv, targets):
        for target in targets:
            pltpu.make_async_remote_copy(
                src_ref=box.at[sweep, mine],
                dst_ref=box.at[sweep, mine],
                send_sem=send.at[0],
                recv_sem=recv.at[sweep],
                device_id=target,
                device_id_type=MESH,
            ).start()
        wait_bytes(box.at[sweep, pl.ds(0, len(targets))], recv.at[sweep])
        logs = box[sweep]
        top = jnp.max(logs, axis=0)
        return top + jnp.log2(jnp.sum(jnp.exp2(logs - top[None]), axis=0))

    def gamma_row(gamma):
        return jnp.concatenate([gamma[t : t + 1, :] for t in range(TILES)], axis=1)

    def sweep_body(sweep, gamma):
        for tile in range(TILES):
            column = []
            for start in range(tile * LANES, (tile + 1) * LANES, CHUNK):
                values = cost_ref[pl.ds(start, CHUNK), :] + gamma_row(gamma)
                top = jnp.max(values, axis=1, keepdims=True)
                summed = jnp.sum(jnp.exp2(values - top), axis=1, keepdims=True)
                column.append(jnp.broadcast_to(top + jnp.log2(summed), (CHUNK, LANES)))
            column = jnp.concatenate(column, axis=0)
            row_box[sweep, col, pl.ds(tile, 1), :] = jnp.sum(
                jnp.where(diag, column, 0.0), axis=0, keepdims=True
            )
        lse = exchange(
            row_box, col, sweep, row_send, row_recv, [(row, peer) for peer in row_peers]
        )
        rho = jnp.where(live_row, -log_one - lse, 0.0)
        vectors_ref[pl.ds(0, TILES), :] = rho
        for tile in range(TILES):
            spread = jnp.broadcast_to(rho[tile : tile + 1, :], (LANES, LANES))
            rho_ref[pl.ds(tile * LANES, LANES), :] = jnp.broadcast_to(
                jnp.sum(jnp.where(diag, spread, 0.0), axis=1, keepdims=True), (LANES, LANES)
            )
        for tile in range(TILES):
            lanes = pl.ds(tile * LANES, LANES)
            tops, sums = [], []
            for start in range(0, BLOCK, 2 * CHUNK):
                rows = pl.ds(start, 2 * CHUNK)
                values = (cost_ref[rows, lanes] + rho_ref[rows, :]).reshape(
                    2 * CHUNK // 8, 8, LANES
                )
                top = jnp.max(values, axis=0)
                tops.append(top)
                sums.append(jnp.sum(jnp.exp2(values - top[None]), axis=0))
            high = functools.reduce(jnp.maximum, tops)
            high = jnp.max(high, axis=0, keepdims=True)
            summed = sum(s * jnp.exp2(t - high) for s, t in zip(sums, tops))
            col_box[sweep, row, pl.ds(tile, 1), :] = high + jnp.log2(
                jnp.sum(summed, axis=0, keepdims=True)
            )
        lse = exchange(
            col_box, row, sweep, col_send, col_recv, [(peer, col) for peer in col_peers]
        )
        return jnp.where(live_col, -log_two - lse, 0.0)

    gamma = lax.fori_loop(0, SWEEPS, sweep_body, jnp.zeros((TILES, LANES), jnp.float32))

    unit = jnp.float32(math.log(2.0) / math.sqrt(mass_scale))
    rho = vectors_ref[pl.ds(0, TILES), :]
    row_const = vectors_ref[pl.ds(8, TILES), :] / all_one
    col_const = vectors_ref[pl.ds(12, TILES), :] / all_two
    vectors_ref[pl.ds(4, TILES), :] = gamma
    vectors_ref[pl.ds(8, TILES), :] = jnp.where(live_row, rho * unit + row_const, 0.0)
    vectors_ref[pl.ds(12, TILES), :] = jnp.where(live_col, gamma * unit + col_const, 0.0)

    wait_bytes(row_box.at[:, pl.ds(0, 3)], row_send.at[0])
    wait_bytes(col_box.at[:, pl.ds(0, 31)], col_send.at[0])
    for part in range(PARTS):
        wait_bytes(plans[part].at[pl.ds(0, 31)], plan_send.at[part])
        wait_bytes(firsts[part].at[pl.ds(0, 3)], first_send.at[part])


def finish_kernel(mass_scale, cost_ref, rho_ref, vectors_ref, plan_ref, row_ref, col_ref):
    gamma = jnp.concatenate([vectors_ref[pl.ds(4 + t, 1), :] for t in range(TILES)], axis=1)
    for start in range(0, BLOCK, CHUNK):
        rows = pl.ds(start, CHUNK)
        exponent = (
            cost_ref[rows, :] + jnp.concatenate([rho_ref[rows, :]] * TILES, axis=1) + gamma
        )
        plan_ref[rows, :] = jnp.float32(mass_scale) * jnp.exp2(exponent)
    row_ref[...] = vectors_ref[pl.ds(8, TILES), :]
    col_ref[...] = vectors_ref[pl.ds(12, TILES), :]


def body(graph_one, graph_two, coupling, sizes_one, sizes_two):
    graph_one, graph_two, coupling, sizes_one, sizes_two = (
        pltpu.with_memory_space_constraint(value, pltpu.HBM)
        for value in (graph_one, graph_two, coupling, sizes_one, sizes_two)
    )
    mass_scale = float(graph_one.shape[1] * graph_two.shape[1])
    vmem = pl.BlockSpec(memory_space=pltpu.VMEM)
    smem = pl.BlockSpec(memory_space=pltpu.SMEM)
    hbm = pl.BlockSpec(memory_space=pltpu.HBM)
    f32, bf16 = jnp.float32, jnp.bfloat16
    dma = pltpu.SemaphoreType.DMA
    cost, rho, vectors = pl.pallas_call(
        functools.partial(gw_kernel, mass_scale),
        out_shape=(
            jax.ShapeDtypeStruct((BLOCK, BLOCK), f32),
            jax.ShapeDtypeStruct((BLOCK, LANES), f32),
            jax.ShapeDtypeStruct((4 * TILES, LANES), f32),
        ),
        in_specs=[hbm, hbm, hbm, smem, smem],
        out_specs=(vmem, vmem, vmem),
        scratch_shapes=[
            pltpu.VMEM((32, BLOCK, WIDTHS[0]), bf16),
            pltpu.VMEM((32, BLOCK, WIDTHS[1]), bf16),
            pltpu.VMEM((4, BLOCK, WIDTHS[0]), bf16),
            pltpu.VMEM((4, BLOCK, WIDTHS[1]), bf16),
            pltpu.VMEM((BLOCK, WIDTHS[0]), f32),
            pltpu.VMEM((BLOCK, WIDTHS[1]), f32),
            pltpu.VMEM((32, BLOCK, BLOCK), bf16),
            pltpu.VMEM((4, BLOCK, BLOCK), bf16),
            pltpu.VMEM((BLOCK, BLOCK), f32),
            pltpu.VMEM((BLOCK, LANES), f32),
            pltpu.VMEM((SWEEPS, 4, TILES, LANES), f32),
            pltpu.VMEM((SWEEPS, 32, TILES, LANES), f32),
            dma((2,)),
            dma((len(STEPS),)),
            dma((PARTS,)),
            dma((len(plan_of_moves()[1]),)),
            dma((PARTS, len(STEPS))),
            dma((PARTS,)),
            dma((PARTS, 6)),
            dma((1,)),
            dma((SWEEPS,)),
            dma((1,)),
            dma((SWEEPS,)),
        ],
        compiler_params=pltpu.CompilerParams(
            collective_id=0, has_side_effects=True, vmem_limit_bytes=52000 * 1024
        ),
        name="gw_step",
    )(graph_one, graph_two, coupling, sizes_one, sizes_two)
    plan, row_potential, col_potential = pl.pallas_call(
        functools.partial(finish_kernel, mass_scale),
        out_shape=(
            jax.ShapeDtypeStruct((BLOCK, BLOCK), f32),
            jax.ShapeDtypeStruct((TILES, LANES), f32),
            jax.ShapeDtypeStruct((TILES, LANES), f32),
        ),
        in_specs=[vmem, vmem, vmem],
        out_specs=(vmem, vmem, vmem),
        compiler_params=pltpu.CompilerParams(vmem_limit_bytes=8 * 1024 * 1024),
        name="finish",
    )(cost, rho, vectors)
    return plan, row_potential.reshape(BLOCK), col_potential.reshape(BLOCK)


def solution(mesh):
    return jax.shard_map(
        body,
        mesh=mesh,
        in_specs=(P("row", None), P("col", None), P("row", "col"), P(), P()),
        out_specs=(P("row", "col"), P("row"), P("col")),
        check_vma=False,
    )
```

```python
import functools
import math

import jax
import jax.numpy as jnp
from jax import lax
from jax.experimental import pallas as pl
from jax.experimental.pallas import tpu as pltpu
from jax.sharding import PartitionSpec as P

BLOCK = 512
SWEEPS = 5
LANES = 128
TILES = BLOCK // LANES
CHUNK = 64
WIDTHS = (384, 128)
BEGINS = (0, 384)
PARTS = len(WIDTHS)
OFFSETS = (0, -1, 1, 2)
STEPS = tuple((first, second) for second in OFFSETS for first in OFFSETS)
HALF = BLOCK // 2
UNIT = BLOCK // 4
AFTER = ((7, 40),)
LAG = 1
LOOPED = 5
CUTS = (1, 2)
MESH = pl.DeviceIdType.MESH

very_low = -1e30


def plane_neighbours():
    steps = []
    for dx in range(4):
        for dz in range(4):
            for dc in range(2):
                if dx or dz or dc:
                    far = min(dx, 4 - dx) + min(dz, 4 - dz)
                    steps.append((-far, -dc, dx, dz, dc))
    return [step[2:] for step in sorted(steps)]


def diagonal():
    return lax.broadcasted_iota(jnp.int32, (LANES, LANES), 0) == lax.broadcasted_iota(
        jnp.int32, (LANES, LANES), 1
    )


COLUMN_US, HOP_US, SLOT_US, AHEAD_US = 1.405 / 256, 2.5, 1.0, 2.8


def sends_of(part, half, turn, first, second):
    onward = 1 if turn == 0 else -1
    out = []
    if second == 0:
        if first == 0:
            for way in (1, -1):
                out.append((0, way, (-way, 0), 4 if way == onward else 3))
        elif first == -onward:
            out.append((0, onward, (2, 0), 3))
        for way in (1, -1):
            out.append((1, way, (first, -way), 2 if way == onward else 1))
    elif second == -onward:
        out.append((1, onward, (first, 2), 1))
    return out


def timetable():
    arrival = {
        (part, half, turn, 0, 0): 0.0
        for part in range(PARTS)
        for half in range(2)
        for turn in range(2)
    }
    free = {(axis, way): 0.0 for axis in range(2) for way in (1, -1)}
    pending, known, slots, now = [], set(), [], 0.0
    while len(known) < PARTS * 4 * len(STEPS):
        fresh = sorted(
            (unit for unit in arrival if arrival[unit] <= now and unit not in known),
            key=lambda unit: (arrival[unit], unit),
        )
        known.update(fresh)
        for unit in fresh:
            pending += [(unit, *send) for send in sends_of(*unit)]
        sends = []
        for axis, way in free:
            while max(free[axis, way], now) - now < AHEAD_US:
                ready = [
                    send
                    for send in pending
                    if send[2] == way and (send[1] + send[0][1]) % 2 == axis
                ]
                if not ready:
                    break
                best = min(ready, key=lambda send: (send[0][0], -send[4]))
                pending.remove(best)
                free[axis, way] = (
                    max(free[axis, way], now) + COLUMN_US * WIDTHS[best[0][0]]
                )
                arrival[best[0][:3] + best[3]] = free[axis, way] + HOP_US
                sends.append(best)
        slots.append((fresh, sends))
        now += SLOT_US
    return slots


def group_of(unit):
    part, half, turn, first, second = unit
    if second == 2:
        return (part, first, second)
    if second and second != (-1 if turn == 0 else 1):
        return (part, turn, first, second)
    return unit


def grouped(slots):
    size, seen, out = {}, {}, []
    for fresh, _ in slots:
        for unit in fresh:
            size[group_of(unit)] = size.get(group_of(unit), 0) + 1
    for fresh, sends in slots:
        ready = []
        for unit in fresh:
            group = group_of(unit)
            seen.setdefault(group, []).append(unit)
            if len(seen[group]) == size[group]:
                ready.append((group, seen[group]))
        out.append((ready, sends))
    groups = [group for group in size if group[-2:] != (0, 0)]
    return out, {group: index for index, group in enumerate(groups)}


def items_of(slots):
    count, work, last = {}, {}, -1
    for index, (ready, _) in enumerate(slots):
        for part, _, _, first, second in (unit for _, units in ready for unit in units):
            key = (part, STEPS.index((first, second)))
            count[key] = count.get(key, 0) + 1
            if count[key] == 4:
                last = max(2 * (index + LAG), last + 1)
                work[last] = key
    return work


def plan_of_moves():
    return grouped(timetable())


def gw_kernel(
    mass_scale,
    graph_one_ref,
    graph_two_ref,
    coupling_ref,
    sizes_one_ref,
    sizes_two_ref,
    cost_ref,
    rho_ref,
    vectors_ref,
    *scratch,
):
    (
        plan_wide,
        plan_slim,
        first_wide,
        first_slim,
        total_wide,
        total_slim,
        one_ref,
        two_ref,
        loaded_ref,
        squares_ref,
        row_box,
        col_box,
        load_sem,
        one_sem,
        plan_send,
        plan_recv,
        pair_recv,
        first_send,
        first_recv,
        row_send,
        row_recv,
        col_send,
        col_recv,
    ) = scratch
    plans = [plan_wide, plan_slim]
    firsts = [first_wide, first_slim]
    totals = [total_wide, total_slim]
    load_coupling = pltpu.make_async_copy(coupling_ref, loaded_ref, load_sem.at[0])
    load_coupling.start()
    row = lax.axis_index("row")
    col = lax.axis_index("col")
    x, z, core = row // 8, (row // 2) % 4, row % 2
    other = 1 - core
    partner = row + 1 - 2 * core

    def around(value):
        return [value] + [
            jnp.where(value >= 4 - step, value + step - 4, value + step) for step in (1, 2, 3)
        ]

    xs, zs = [8 * value for value in around(x)], [2 * value for value in around(z)]
    _, up, across, down = around(col)
    row_peers = [across, up, down]
    col_peers = [
        xs[dx] + zs[dz] + (other if dc else core) for dx, dz, dc in plane_neighbours()
    ]
    places = [[xs[dx] + zs[dz] + core for dz in range(4)] for dx in range(4)]

    barrier = pltpu.get_barrier_semaphore()
    for peer in (up, down):
        pl.semaphore_signal(barrier, inc=1, device_id=(row, peer), device_id_type=MESH)
    for peer in (places[1][0], places[3][0], places[0][1], places[0][3], partner):
        pl.semaphore_signal(barrier, inc=1, device_id=(peer, col), device_id_type=MESH)

    load_two = []
    for block in range(4):
        load_two.append(
            pltpu.make_async_copy(
                graph_two_ref.at[:, pl.ds(block * BLOCK, BLOCK)], two_ref.at[block], load_sem.at[1]
            )
        )
    size_one = sizes_one_ref[row]
    size_two = sizes_two_ref[col]
    slot = lax.broadcasted_iota(jnp.int32, (TILES, LANES), 0) * LANES + lax.broadcasted_iota(
        jnp.int32, (TILES, LANES), 1
    )
    live_row = slot < size_one
    live_col = slot < size_two
    diag = diagonal()

    def live_part(start, width, offset=0):
        ids = lax.broadcasted_iota(jnp.int32, (CHUNK, width), 0) + start
        lanes = lax.broadcasted_iota(jnp.int32, (CHUNK, width), 1) + offset
        return (ids < size_one) & (lanes < size_two)

    load_coupling.wait()
    for start in range(0, BLOCK, CHUNK):
        rows = pl.ds(start, CHUNK)
        for part in range(PARTS):
            kept = jnp.where(
                live_part(start, WIDTHS[part], BEGINS[part]),
                loaded_ref[rows, pl.ds(BEGINS[part], WIDTHS[part])],
                0.0,
            )
            plans[part][row, rows, :] = kept.astype(jnp.bfloat16)
    squares_ref[...] = jnp.zeros_like(squares_ref)
    pl.semaphore_wait(barrier, 7)

    def place(half, first, second):
        dx, dz = (first, second) if half == 0 else (second, first)
        return places[dx % 4][dz % 4]

    def wait_bytes(ref, sem):
        pltpu.make_async_copy(ref, ref, sem).wait()

    def piece_of(part, half, turn, first, second):
        rows = pl.ds(half * HALF + turn * UNIT, UNIT)
        return plans[part].at[place(half, first, second), rows, :]

    def moves(ready, sends, fetched):
        for group, units in ready:
            if group in semaphores:
                rows = pl.ds(0, UNIT * len(units))
                wait_bytes(plans[group[0]].at[0, rows, :], plan_recv.at[semaphores[group]])
        for unit, axis, way, seen, _ in sends:
            part, half, turn, first, second = unit
            piece = piece_of(*unit)
            target = place(half, way, 0) if axis == 0 else place(half, 0, way)
            pltpu.make_async_remote_copy(
                src_ref=piece,
                dst_ref=piece,
                send_sem=plan_send.at[part],
                recv_sem=plan_recv.at[semaphores[group_of((part, half, turn, *seen))]],
                device_id=(target, col),
                device_id_type=MESH,
            ).start()
        for unit in (unit for _, units in ready for unit in units):
            part, half, turn, first, second = unit
            piece = piece_of(*unit)
            pltpu.make_async_remote_copy(
                src_ref=piece,
                dst_ref=piece,
                send_sem=plan_send.at[part],
                recv_sem=pair_recv.at[part, STEPS.index((first, second))],
                device_id=(partner, col),
                device_id_type=MESH,
            ).start()
        for step in fetched:
            for half in range(2):
                for owner in (core, other):
                    source = place(half, *STEPS[step]) - core + owner
                    start = pl.multiple_of(source * BLOCK + half * HALF, HALF)
                    pltpu.make_async_copy(
                        graph_one_ref.at[:, pl.ds(start, HALF)],
                        one_ref.at[source, :, pl.ds(half * HALF, HALF)],
                        one_sem.at[step],
                    ).start()

    def pick(options, index):
        value = options[OFFSETS[-1] % 4]
        for place_of, offset in enumerate(OFFSETS[:-1]):
            value = jnp.where(index == place_of, options[offset % 4], value)
        return value

    def add_products(plan, total_ref, chips):
        for start in range(0, BLOCK, HALF):
            total = total_ref[pl.ds(start, HALF), :]
            for half in range(2):
                rows = pl.ds(half * HALF, HALF)
                for owner in (core, other):
                    source = chips[half] + owner
                    total = total + jnp.dot(
                        one_ref[source, pl.ds(start, HALF), rows],
                        plan[source, rows, :],
                        preferred_element_type=jnp.float32,
                    )
            total_ref[pl.ds(start, HALF), :] = total

    def multiply_slim(step, chips):
        wait_bytes(plan_slim.at[0], pair_recv.at[1, step])
        add_products(plan_slim, total_slim, chips)

    def multiply(code):
        part = jnp.where(code >= len(STEPS), 1, 0)
        step = code - len(STEPS) * part
        second = (
            jnp.where(step >= 4, 1, 0) + jnp.where(step >= 8, 1, 0) + jnp.where(step >= 12, 1, 0)
        )
        first = step - 4 * second
        chips = (pick(xs, first) + pick(zs, second), pick(xs, second) + pick(zs, first))

        @pl.when(part > 0)
        def _():
            multiply_slim(step, chips)

        @pl.when(part == 0)
        def _():
            wait_bytes(plan_wide.at[0], pair_recv.at[part, step])
            wait_bytes(one_ref.at[pl.ds(0, 2)], one_sem.at[step])
            add_products(plan_wide, total_wide, chips)
            for start in range(0, BLOCK, CHUNK):
                squares = squares_ref[pl.ds(start, CHUNK), :]
                for half in range(2):
                    for owner in (core, other):
                        source = chips[half] + owner
                        size = sizes_one_ref[source]
                        for tile in range(2):
                            lanes = half * HALF + tile * LANES
                            ids = lax.broadcasted_iota(jnp.int32, (CHUNK, LANES), 1) + lanes
                            value = one_ref[
                                source, pl.ds(start, CHUNK), pl.ds(lanes, LANES)
                            ].astype(jnp.float32)
                            squares = squares + jnp.where(ids < size, value * value, 0.0)
                squares_ref[pl.ds(start, CHUNK), :] = squares

    def first_rows(part, half, cut):
        if cut is None:
            return pl.ds(half * HALF, HALF)
        count = HALF // CUTS[part]
        return pl.ds(half * HALF + cut * count, count)

    def first_copy(part, half, cut, source, key, target):
        piece = firsts[part].at[source, first_rows(part, half, cut), :]
        pltpu.make_async_remote_copy(
            src_ref=piece,
            dst_ref=piece,
            send_sem=first_send.at[part],
            recv_sem=first_recv.at[part, key],
            device_id=(row, target),
            device_id_type=MESH,
        ).start()

    def first_start(part):
        for start in range(0, BLOCK, CHUNK):
            rows = pl.ds(start, CHUNK)
            firsts[part][col, rows, :] = totals[part][rows, :].astype(jnp.bfloat16)
        for cut in range(CUTS[part]):
            first_copy(part, 0, cut, col, 4 + 2 * cut, up)
            first_copy(part, 1, cut, col, 5 + 2 * cut, down)
        first_copy(part, 1, None, col, 0, up)
        first_copy(part, 0, None, col, 1, down)

    def first_wait(part, half, cut, source, key):
        piece = firsts[part].at[source, first_rows(part, half, cut), :]
        wait_bytes(piece, first_recv.at[part, key])

    def first_onward(part):
        for cut in range(CUTS[part]):
            first_wait(part, 0, cut, down, 4 + 2 * cut)
            first_copy(part, 0, cut, down, 2, up)
            first_wait(part, 1, cut, up, 5 + 2 * cut)
            first_copy(part, 1, cut, up, 3, down)

    def cross_add(part, source, fresh=False):
        added = lax.dot_general(
            firsts[part][source],
            two_ref[source, :, pl.ds(BEGINS[part], WIDTHS[part])],
            (((1,), (1,)), ((), ())),
            preferred_element_type=jnp.float32,
        )
        if fresh:
            cost_ref[...] = added
        else:
            cost_ref[...] += added

    def first_end(part):
        cross_add(part, col, fresh=part == 0)
        first_wait(part, 1, None, down, 0)
        cross_add(part, down)
        first_wait(part, 0, None, up, 1)
        cross_add(part, up)
        first_wait(part, 0, None, across, 2)
        first_wait(part, 1, None, across, 3)
        cross_add(part, across)

    def square_columns():
        wait_bytes(two_ref, load_sem.at[1])
        col_square = []
        for tile in range(TILES):
            summed = []
            for start in range(tile * LANES, (tile + 1) * LANES, CHUNK):
                gathered = jnp.zeros((CHUNK, LANES), jnp.float32)
                for block in range(4):
                    for lane in range(TILES):
                        ids = lax.broadcasted_iota(jnp.int32, (CHUNK, LANES), 1) + lane * LANES
                        value = two_ref[block, pl.ds(start, CHUNK), pl.ds(lane * LANES, LANES)].astype(
                            jnp.float32
                        )
                        gathered = gathered + jnp.where(
                            ids < sizes_two_ref[block], value * value, 0.0
                        )
                summed.append(
                    jnp.broadcast_to(jnp.sum(gathered, axis=1, keepdims=True), (CHUNK, LANES))
                )
            vectors_ref[pl.ds(12 + tile, 1), :] = jnp.sum(
                jnp.where(diag, jnp.concatenate(summed, axis=0), 0.0), axis=0, keepdims=True
            )

    slots, semaphores = plan_of_moves()
    work = items_of(slots)
    length = max(work) // 2 + 1
    looped = max(turn // 2 for turn in work if work[turn][0] == 0) + 1 + LOOPED
    slots = slots + [([], [])] * (length - len(slots))
    order = [work[turn][1] for turn in sorted(work) if work[turn][0] == 0]
    fetches = [order[:4]] + [[step] for step in order[4:]] + [[]] * length
    whole = [max(turn // 2 for turn in work if work[turn][0] == part) for part in range(PARTS)]
    extra = {5: [square_columns]}
    for part in range(PARTS - 1):
        for after, run in zip(AFTER[part], (first_onward, first_end)):
            extra.setdefault(min(whole[part] + after, length), []).append(
                functools.partial(run, part)
            )
    for total in totals:
        total[...] = jnp.zeros_like(total)
    moves(*slots[0], fetches[0])
    for copy in load_two:
        copy.start()
    total_one = jnp.float32(0)
    for block in range(sizes_one_ref.shape[0]):
        total_one = total_one + sizes_one_ref[block].astype(jnp.float32)
    total_two = jnp.float32(0)
    for block in range(sizes_two_ref.shape[0]):
        total_two = total_two + sizes_two_ref[block].astype(jnp.float32)
    all_one = jnp.full((TILES, LANES), total_one, jnp.float32)
    all_two = jnp.full((TILES, LANES), total_two, jnp.float32)
    log_one = jnp.log2(all_one)
    log_two = jnp.log2(all_two)
    def one_slot(slot, carry):
        for group in range(0, looped, 8):

            @pl.when((slot >= group) & (slot < group + 8))
            def _():
                for index in range(max(group, 1), min(group + 8, looped)):
                    if slots[index] != ([], []) or fetches[index] or index in extra:

                        @pl.when(slot == index)
                        def _():
                            moves(*slots[index], fetches[index])
                            for run in extra.get(index, ()):
                                run()

        def one_turn(turn, carry):
            code = jnp.int32(-1)
            for index, (part, step) in work.items():
                if index >= 2 * looped:
                    continue
                code = jnp.where(2 * slot + turn == index, part * len(STEPS) + step, code)

            @pl.when(code >= 0)
            def _():
                multiply(code)

            return carry

        lax.fori_loop(0, 2, one_turn, 0)
        for part in range(PARTS - 1):

            @pl.when(slot == whole[part])
            def _():
                first_start(part)

        return carry

    lax.fori_loop(0, looped, one_slot, 0)
    for index in range(looped, length):
        moves(*slots[index], fetches[index])
        for run in extra.get(index, ()):
            run()
        for turn in (2 * index, 2 * index + 1):
            if turn in work:
                step = work[turn][1]
                multiply_slim(step, [place(half, *STEPS[step]) - core for half in range(2)])
    first_start(PARTS - 1)
    for run in extra.get(length, ()):
        run()
    for tile in range(TILES):
        column = jnp.broadcast_to(
            jnp.sum(squares_ref[pl.ds(tile * LANES, LANES), :], axis=1, keepdims=True),
            (LANES, LANES),
        )
        vectors_ref[pl.ds(8 + tile, 1), :] = jnp.sum(
            jnp.where(diag, column, 0.0), axis=0, keepdims=True
        )
    first_onward(PARTS - 1)
    first_end(PARTS - 1)

    scale = jnp.float32(2.0 / math.sqrt(mass_scale) * math.log2(math.e))
    for start in range(0, BLOCK, CHUNK):
        rows = pl.ds(start, CHUNK)
        cost_ref[rows, :] = jnp.where(
            live_part(start, BLOCK), cost_ref[rows, :] * scale, jnp.float32(very_low)
        )

    def exchange(box, mine, sweep, send, recv, targets):
        for target in targets:
            pltpu.make_async_remote_copy(
                src_ref=box.at[sweep, mine],
                dst_ref=box.at[sweep, mine],
                send_sem=send.at[0],
                recv_sem=recv.at[sweep],
                device_id=target,
                device_id_type=MESH,
            ).start()
        wait_bytes(box.at[sweep, pl.ds(0, len(targets))], recv.at[sweep])
        logs = box[sweep]
        top = jnp.max(logs, axis=0)
        return top + jnp.log2(jnp.sum(jnp.exp2(logs - top[None]), axis=0))

    def gamma_row(gamma):
        return jnp.concatenate([gamma[t : t + 1, :] for t in range(TILES)], axis=1)

    def sweep_body(sweep, gamma):
        lines = []
        for tile in range(TILES):
            column = []
            for start in range(tile * LANES, (tile + 1) * LANES, CHUNK):
                values = cost_ref[pl.ds(start, CHUNK), :] + gamma_row(gamma)
                top = jnp.max(values, axis=1, keepdims=True)
                summed = jnp.sum(jnp.exp2(values - top), axis=1, keepdims=True)
                column.append(jnp.broadcast_to(top + jnp.log2(summed), (CHUNK, LANES)))
            column = jnp.concatenate(column, axis=0)
            lines.append(jnp.sum(jnp.where(diag, column, 0.0), axis=0, keepdims=True))
        row_box[sweep, col] = jnp.concatenate(lines, axis=0)
        lse = exchange(
            row_box, col, sweep, row_send, row_recv, [(row, peer) for peer in row_peers]
        )
        rho = jnp.where(live_row, -log_one - lse, 0.0)
        vectors_ref[pl.ds(0, TILES), :] = rho
        columns = []
        for tile in range(TILES):
            spread = jnp.broadcast_to(rho[tile : tile + 1, :], (LANES, LANES))
            columns.append(
                jnp.sum(jnp.where(diag, spread, 0.0), axis=1, keepdims=True)
            )
        for tile in range(TILES):
            rho_ref[pl.ds(tile * LANES, LANES), :] = jnp.broadcast_to(
                columns[tile], (LANES, LANES)
            )
        lines = []
        for tile in range(TILES):
            lanes = pl.ds(tile * LANES, LANES)
            tops, sums = [], []
            for start in range(0, BLOCK, 2 * CHUNK):
                rows = pl.ds(start, 2 * CHUNK)
                values = (cost_ref[rows, lanes] + rho_ref[rows, :]).reshape(
                    2 * CHUNK // 8, 8, LANES
                )
                top = jnp.max(values, axis=0)
                tops.append(top)
                sums.append(jnp.sum(jnp.exp2(values - top[None]), axis=0))
            high = functools.reduce(jnp.maximum, tops)
            high = jnp.max(high, axis=0, keepdims=True)
            summed = sum(s * jnp.exp2(t - high) for s, t in zip(sums, tops))
            lines.append(high + jnp.log2(jnp.sum(summed, axis=0, keepdims=True)))
        col_box[sweep, row] = jnp.concatenate(lines, axis=0)
        lse = exchange(
            col_box, row, sweep, col_send, col_recv, [(peer, col) for peer in col_peers]
        )
        return jnp.where(live_col, -log_two - lse, 0.0)

    gamma = lax.fori_loop(0, SWEEPS, sweep_body, jnp.zeros((TILES, LANES), jnp.float32))

    unit = jnp.float32(math.log(2.0) / math.sqrt(mass_scale))
    rho = vectors_ref[pl.ds(0, TILES), :]
    row_const = vectors_ref[pl.ds(8, TILES), :] / all_one
    col_const = vectors_ref[pl.ds(12, TILES), :] / all_two
    vectors_ref[pl.ds(4, TILES), :] = gamma
    vectors_ref[pl.ds(8, TILES), :] = jnp.where(live_row, rho * unit + row_const, 0.0)
    vectors_ref[pl.ds(12, TILES), :] = jnp.where(live_col, gamma * unit + col_const, 0.0)

    wait_bytes(row_box.at[:, pl.ds(0, 3)], row_send.at[0])
    wait_bytes(col_box.at[:, pl.ds(0, 31)], col_send.at[0])
    for part in range(PARTS):
        wait_bytes(plans[part].at[pl.ds(0, 31)], plan_send.at[part])
        wait_bytes(firsts[part].at[pl.ds(0, 3)], first_send.at[part])


def finish_kernel(
    mass_scale, cost_ref, rho_ref, vectors_ref, plan_ref, row_ref, col_ref, made_ref, made_sem
):
    gamma = jnp.concatenate([vectors_ref[pl.ds(4 + t, 1), :] for t in range(TILES)], axis=1)
    copies = []
    for start in range(0, BLOCK, LANES):
        rows = pl.ds(start, LANES)
        exponent = (
            cost_ref[rows, :] + jnp.concatenate([rho_ref[rows, :]] * TILES, axis=1) + gamma
        )
        made_ref[rows, :] = jnp.float32(mass_scale) * jnp.exp2(exponent)
        copy = pltpu.make_async_copy(
            made_ref.at[rows, :], plan_ref.at[rows, :], made_sem.at[start // LANES]
        )
        copy.start()
        copies.append(copy)
    row_ref[...] = vectors_ref[pl.ds(8, TILES), :]
    col_ref[...] = vectors_ref[pl.ds(12, TILES), :]
    for copy in copies:
        copy.wait()


def body(graph_one, graph_two, coupling, sizes_one, sizes_two):
    graph_one, graph_two, coupling, sizes_one, sizes_two = (
        pltpu.with_memory_space_constraint(value, pltpu.HBM)
        for value in (graph_one, graph_two, coupling, sizes_one, sizes_two)
    )
    mass_scale = float(graph_one.shape[1] * graph_two.shape[1])
    vmem = pl.BlockSpec(memory_space=pltpu.VMEM)
    smem = pl.BlockSpec(memory_space=pltpu.SMEM)
    hbm = pl.BlockSpec(memory_space=pltpu.HBM)
    f32, bf16 = jnp.float32, jnp.bfloat16
    dma = pltpu.SemaphoreType.DMA
    cost, rho, vectors = pl.pallas_call(
        functools.partial(gw_kernel, mass_scale),
        out_shape=(
            jax.ShapeDtypeStruct((BLOCK, BLOCK), f32),
            jax.ShapeDtypeStruct((BLOCK, LANES), f32),
            jax.ShapeDtypeStruct((4 * TILES, LANES), f32),
        ),
        in_specs=[hbm, hbm, hbm, smem, smem],
        out_specs=(vmem, vmem, vmem),
        scratch_shapes=[
            pltpu.VMEM((32, BLOCK, WIDTHS[0]), bf16),
            pltpu.VMEM((32, BLOCK, WIDTHS[1]), bf16),
            pltpu.VMEM((4, BLOCK, WIDTHS[0]), bf16),
            pltpu.VMEM((4, BLOCK, WIDTHS[1]), bf16),
            pltpu.VMEM((BLOCK, WIDTHS[0]), f32),
            pltpu.VMEM((BLOCK, WIDTHS[1]), f32),
            pltpu.VMEM((32, BLOCK, BLOCK), bf16),
            pltpu.VMEM((4, BLOCK, BLOCK), bf16),
            pltpu.VMEM((BLOCK, BLOCK), f32),
            pltpu.VMEM((BLOCK, LANES), f32),
            pltpu.VMEM((SWEEPS, 4, TILES, LANES), f32),
            pltpu.VMEM((SWEEPS, 32, TILES, LANES), f32),
            dma((2,)),
            dma((len(STEPS),)),
            dma((PARTS,)),
            dma((len(plan_of_moves()[1]),)),
            dma((PARTS, len(STEPS))),
            dma((PARTS,)),
            dma((PARTS, 4 + 2 * max(CUTS))),
            dma((1,)),
            dma((SWEEPS,)),
            dma((1,)),
            dma((SWEEPS,)),
        ],
        compiler_params=pltpu.CompilerParams(
            collective_id=0, has_side_effects=True, vmem_limit_bytes=52000 * 1024
        ),
        name="gw_step",
    )(graph_one, graph_two, coupling, sizes_one, sizes_two)
    plan, row_potential, col_potential = pl.pallas_call(
        functools.partial(finish_kernel, mass_scale),
        out_shape=(
            jax.ShapeDtypeStruct((BLOCK, BLOCK), f32),
            jax.ShapeDtypeStruct((TILES, LANES), f32),
            jax.ShapeDtypeStruct((TILES, LANES), f32),
        ),
        in_specs=[vmem, vmem, vmem],
        out_specs=(hbm, vmem, vmem),
        scratch_shapes=[pltpu.VMEM((BLOCK, BLOCK), f32), dma((TILES,))],
        compiler_params=pltpu.CompilerParams(vmem_limit_bytes=8 * 1024 * 1024),
        name="finish",
    )(cost, rho, vectors)
    return plan, row_potential.reshape(BLOCK), col_potential.reshape(BLOCK)


def solution(mesh):
    return jax.shard_map(
        body,
        mesh=mesh,
        in_specs=(P("row", None), P("col", None), P("row", "col"), P(), P()),
        out_specs=(P("row", "col"), P("row"), P("col")),
        check_vma=False,
    )
```

```python
import functools
import math

import jax
import jax.numpy as jnp
from jax import lax
from jax.experimental import pallas as pl
from jax.experimental.pallas import tpu as pltpu
from jax.sharding import PartitionSpec as P

BLOCK = 512
SWEEPS = 5
LANES = 128
TILES = BLOCK // LANES
CHUNK = 64
WIDTHS = (384, 128)
BEGINS = (0, 384)
PARTS = len(WIDTHS)
OFFSETS = (0, -1, 1, 2)
STEPS = tuple((first, second) for second in OFFSETS for first in OFFSETS)
HALF = BLOCK // 2
UNIT = BLOCK // 4
AFTER = ((7, 40),)
LAG = 1
LOOPED = 5
CUTS = (1, 4)
MESH = pl.DeviceIdType.MESH

very_low = -1e30


def plane_neighbours():
    steps = []
    for dx in range(4):
        for dz in range(4):
            for dc in range(2):
                if dx or dz or dc:
                    far = min(dx, 4 - dx) + min(dz, 4 - dz)
                    steps.append((-far, -dc, dx, dz, dc))
    return [step[2:] for step in sorted(steps)]


def diagonal():
    return lax.broadcasted_iota(jnp.int32, (LANES, LANES), 0) == lax.broadcasted_iota(
        jnp.int32, (LANES, LANES), 1
    )


COLUMN_US, HOP_US, SLOT_US, AHEAD_US = 1.405 / 256, 2.5, 1.0, 2.8


def sends_of(part, half, turn, first, second):
    onward = 1 if turn == 0 else -1
    out = []
    if second == 0:
        if first == 0:
            for way in (1, -1):
                out.append((0, way, (-way, 0), 4 if way == onward else 3))
        elif first == -onward:
            out.append((0, onward, (2, 0), 3))
        for way in (1, -1):
            out.append((1, way, (first, -way), 2 if way == onward else 1))
    elif second == -onward:
        out.append((1, onward, (first, 2), 1))
    return out


def timetable():
    arrival = {
        (part, half, turn, 0, 0): 0.0
        for part in range(PARTS)
        for half in range(2)
        for turn in range(2)
    }
    free = {(axis, way): 0.0 for axis in range(2) for way in (1, -1)}
    pending, known, slots, now = [], set(), [], 0.0
    while len(known) < PARTS * 4 * len(STEPS):
        fresh = sorted(
            (unit for unit in arrival if arrival[unit] <= now and unit not in known),
            key=lambda unit: (arrival[unit], unit),
        )
        known.update(fresh)
        for unit in fresh:
            pending += [(unit, *send) for send in sends_of(*unit)]
        sends = []
        for axis, way in free:
            while max(free[axis, way], now) - now < AHEAD_US:
                ready = [
                    send
                    for send in pending
                    if send[2] == way and (send[1] + send[0][1]) % 2 == axis
                ]
                if not ready:
                    break
                best = min(ready, key=lambda send: (send[0][0], -send[4]))
                pending.remove(best)
                free[axis, way] = (
                    max(free[axis, way], now) + COLUMN_US * WIDTHS[best[0][0]]
                )
                arrival[best[0][:3] + best[3]] = free[axis, way] + HOP_US
                sends.append(best)
        slots.append((fresh, sends))
        now += SLOT_US
    return slots


def group_of(unit):
    part, half, turn, first, second = unit
    if second == 2:
        return (part, first, second)
    if second and second != (-1 if turn == 0 else 1):
        return (part, turn, first, second)
    return unit


def grouped(slots):
    size, seen, out = {}, {}, []
    for fresh, _ in slots:
        for unit in fresh:
            size[group_of(unit)] = size.get(group_of(unit), 0) + 1
    for fresh, sends in slots:
        ready = []
        for unit in fresh:
            group = group_of(unit)
            seen.setdefault(group, []).append(unit)
            if len(seen[group]) == size[group]:
                ready.append((group, seen[group]))
        out.append((ready, sends))
    groups = [group for group in size if group[-2:] != (0, 0)]
    return out, {group: index for index, group in enumerate(groups)}


def items_of(slots):
    count, work, last = {}, {}, -1
    for index, (ready, _) in enumerate(slots):
        for part, _, _, first, second in (unit for _, units in ready for unit in units):
            key = (part, STEPS.index((first, second)))
            count[key] = count.get(key, 0) + 1
            if count[key] == 4:
                last = max(2 * (index + LAG), last + 1)
                work[last] = key
    return work


def plan_of_moves():
    return grouped(timetable())


def gw_kernel(
    mass_scale,
    graph_one_ref,
    graph_two_ref,
    coupling_ref,
    sizes_one_ref,
    sizes_two_ref,
    cost_ref,
    rho_ref,
    vectors_ref,
    *scratch,
):
    (
        plan_wide,
        plan_slim,
        first_wide,
        first_slim,
        total_wide,
        total_slim,
        one_ref,
        two_ref,
        loaded_ref,
        squares_ref,
        row_box,
        col_box,
        load_sem,
        one_sem,
        plan_send,
        plan_recv,
        pair_recv,
        first_send,
        first_recv,
        row_send,
        row_recv,
        col_send,
        col_recv,
    ) = scratch
    plans = [plan_wide, plan_slim]
    firsts = [first_wide, first_slim]
    totals = [total_wide, total_slim]
    load_coupling = pltpu.make_async_copy(coupling_ref, loaded_ref, load_sem.at[0])
    load_coupling.start()
    row = lax.axis_index("row")
    col = lax.axis_index("col")
    x, z, core = row // 8, (row // 2) % 4, row % 2
    other = 1 - core
    partner = row + 1 - 2 * core

    def around(value):
        return [value] + [
            jnp.where(value >= 4 - step, value + step - 4, value + step) for step in (1, 2, 3)
        ]

    xs, zs = [8 * value for value in around(x)], [2 * value for value in around(z)]
    _, up, across, down = around(col)
    row_peers = [across, up, down]
    col_peers = [
        xs[dx] + zs[dz] + (other if dc else core) for dx, dz, dc in plane_neighbours()
    ]
    places = [[xs[dx] + zs[dz] + core for dz in range(4)] for dx in range(4)]

    barrier = pltpu.get_barrier_semaphore()
    for peer in (up, down):
        pl.semaphore_signal(barrier, inc=1, device_id=(row, peer), device_id_type=MESH)
    for peer in (places[1][0], places[3][0], places[0][1], places[0][3], partner):
        pl.semaphore_signal(barrier, inc=1, device_id=(peer, col), device_id_type=MESH)

    load_two = []
    for block in range(4):
        load_two.append(
            pltpu.make_async_copy(
                graph_two_ref.at[:, pl.ds(block * BLOCK, BLOCK)], two_ref.at[block], load_sem.at[1]
            )
        )
    size_one = sizes_one_ref[row]
    size_two = sizes_two_ref[col]
    slot = lax.broadcasted_iota(jnp.int32, (TILES, LANES), 0) * LANES + lax.broadcasted_iota(
        jnp.int32, (TILES, LANES), 1
    )
    live_row = slot < size_one
    live_col = slot < size_two
    diag = diagonal()

    def live_part(start, width, offset=0):
        ids = lax.broadcasted_iota(jnp.int32, (CHUNK, width), 0) + start
        lanes = lax.broadcasted_iota(jnp.int32, (CHUNK, width), 1) + offset
        return (ids < size_one) & (lanes < size_two)

    load_coupling.wait()
    for start in range(0, BLOCK, CHUNK):
        rows = pl.ds(start, CHUNK)
        for part in range(PARTS):
            kept = jnp.where(
                live_part(start, WIDTHS[part], BEGINS[part]),
                loaded_ref[rows, pl.ds(BEGINS[part], WIDTHS[part])],
                0.0,
            )
            plans[part][row, rows, :] = kept.astype(jnp.bfloat16)
    squares_ref[...] = jnp.zeros_like(squares_ref)
    pl.semaphore_wait(barrier, 7)

    def place(half, first, second):
        dx, dz = (first, second) if half == 0 else (second, first)
        return places[dx % 4][dz % 4]

    def wait_bytes(ref, sem):
        pltpu.make_async_copy(ref, ref, sem).wait()

    def piece_of(part, half, turn, first, second):
        rows = pl.ds(half * HALF + turn * UNIT, UNIT)
        return plans[part].at[place(half, first, second), rows, :]

    def moves(ready, sends, fetched):
        for group, units in ready:
            if group in semaphores:
                rows = pl.ds(0, UNIT * len(units))
                wait_bytes(plans[group[0]].at[0, rows, :], plan_recv.at[semaphores[group]])
        for unit, axis, way, seen, _ in sends:
            part, half, turn, first, second = unit
            piece = piece_of(*unit)
            target = place(half, way, 0) if axis == 0 else place(half, 0, way)
            pltpu.make_async_remote_copy(
                src_ref=piece,
                dst_ref=piece,
                send_sem=plan_send.at[part],
                recv_sem=plan_recv.at[semaphores[group_of((part, half, turn, *seen))]],
                device_id=(target, col),
                device_id_type=MESH,
            ).start()
        for unit in (unit for _, units in ready for unit in units):
            part, half, turn, first, second = unit
            piece = piece_of(*unit)
            pltpu.make_async_remote_copy(
                src_ref=piece,
                dst_ref=piece,
                send_sem=plan_send.at[part],
                recv_sem=pair_recv.at[part, STEPS.index((first, second))],
                device_id=(partner, col),
                device_id_type=MESH,
            ).start()
        for step in fetched:
            for half in range(2):
                for owner in (core, other):
                    source = place(half, *STEPS[step]) - core + owner
                    start = pl.multiple_of(source * BLOCK + half * HALF, HALF)
                    pltpu.make_async_copy(
                        graph_one_ref.at[:, pl.ds(start, HALF)],
                        one_ref.at[source, :, pl.ds(half * HALF, HALF)],
                        one_sem.at[step],
                    ).start()

    def pick(options, index):
        value = options[OFFSETS[-1] % 4]
        for place_of, offset in enumerate(OFFSETS[:-1]):
            value = jnp.where(index == place_of, options[offset % 4], value)
        return value

    def add_products(plan, total_ref, chips):
        for start in range(0, BLOCK, HALF):
            total = total_ref[pl.ds(start, HALF), :]
            for half in range(2):
                rows = pl.ds(half * HALF, HALF)
                for owner in (core, other):
                    source = chips[half] + owner
                    total = total + jnp.dot(
                        one_ref[source, pl.ds(start, HALF), rows],
                        plan[source, rows, :],
                        preferred_element_type=jnp.float32,
                    )
            total_ref[pl.ds(start, HALF), :] = total

    def multiply_slim(step, chips):
        wait_bytes(plan_slim.at[0], pair_recv.at[1, step])
        add_products(plan_slim, total_slim, chips)

    def multiply(code):
        part = jnp.where(code >= len(STEPS), 1, 0)
        step = code - len(STEPS) * part
        second = (
            jnp.where(step >= 4, 1, 0) + jnp.where(step >= 8, 1, 0) + jnp.where(step >= 12, 1, 0)
        )
        first = step - 4 * second
        chips = (pick(xs, first) + pick(zs, second), pick(xs, second) + pick(zs, first))

        @pl.when(part > 0)
        def _():
            multiply_slim(step, chips)

        @pl.when(part == 0)
        def _():
            wait_bytes(plan_wide.at[0], pair_recv.at[part, step])
            wait_bytes(one_ref.at[pl.ds(0, 2)], one_sem.at[step])
            add_products(plan_wide, total_wide, chips)
            for start in range(0, BLOCK, CHUNK):
                squares = squares_ref[pl.ds(start, CHUNK), :]
                for half in range(2):
                    for owner in (core, other):
                        source = chips[half] + owner
                        size = sizes_one_ref[source]
                        for tile in range(2):
                            lanes = half * HALF + tile * LANES
                            ids = lax.broadcasted_iota(jnp.int32, (CHUNK, LANES), 1) + lanes
                            value = one_ref[
                                source, pl.ds(start, CHUNK), pl.ds(lanes, LANES)
                            ].astype(jnp.float32)
                            squares = squares + jnp.where(ids < size, value * value, 0.0)
                squares_ref[pl.ds(start, CHUNK), :] = squares

    def first_rows(part, half, cut):
        if cut is None:
            return pl.ds(half * HALF, HALF)
        count = HALF // CUTS[part]
        return pl.ds(half * HALF + cut * count, count)

    def first_copy(part, half, cut, source, key, target):
        piece = firsts[part].at[source, first_rows(part, half, cut), :]
        pltpu.make_async_remote_copy(
            src_ref=piece,
            dst_ref=piece,
            send_sem=first_send.at[part],
            recv_sem=first_recv.at[part, key],
            device_id=(row, target),
            device_id_type=MESH,
        ).start()

    def first_start(part):
        for start in range(0, BLOCK, CHUNK):
            rows = pl.ds(start, CHUNK)
            firsts[part][col, rows, :] = totals[part][rows, :].astype(jnp.bfloat16)
        for cut in range(CUTS[part]):
            first_copy(part, 0, cut, col, 4 + 2 * cut, up)
            first_copy(part, 1, cut, col, 5 + 2 * cut, down)
        first_copy(part, 1, None, col, 0, up)
        first_copy(part, 0, None, col, 1, down)

    def first_wait(part, half, cut, source, key):
        piece = firsts[part].at[source, first_rows(part, half, cut), :]
        wait_bytes(piece, first_recv.at[part, key])

    def first_onward(part):
        for cut in range(CUTS[part]):
            first_wait(part, 0, cut, down, 4 + 2 * cut)
            first_copy(part, 0, cut, down, 2, up)
            first_wait(part, 1, cut, up, 5 + 2 * cut)
            first_copy(part, 1, cut, up, 3, down)

    def cross_add(part, source, fresh=False):
        added = lax.dot_general(
            firsts[part][source],
            two_ref[source, :, pl.ds(BEGINS[part], WIDTHS[part])],
            (((1,), (1,)), ((), ())),
            preferred_element_type=jnp.float32,
        )
        if fresh:
            cost_ref[...] = added
        else:
            cost_ref[...] += added

    def first_end(part):
        cross_add(part, col, fresh=part == 0)
        first_wait(part, 1, None, down, 0)
        cross_add(part, down)
        first_wait(part, 0, None, up, 1)
        cross_add(part, up)
        first_wait(part, 0, None, across, 2)
        first_wait(part, 1, None, across, 3)
        cross_add(part, across)

    def square_columns():
        wait_bytes(two_ref, load_sem.at[1])
        col_square = []
        for tile in range(TILES):
            summed = []
            for start in range(tile * LANES, (tile + 1) * LANES, CHUNK):
                gathered = jnp.zeros((CHUNK, LANES), jnp.float32)
                for block in range(4):
                    for lane in range(TILES):
                        ids = lax.broadcasted_iota(jnp.int32, (CHUNK, LANES), 1) + lane * LANES
                        value = two_ref[block, pl.ds(start, CHUNK), pl.ds(lane * LANES, LANES)].astype(
                            jnp.float32
                        )
                        gathered = gathered + jnp.where(
                            ids < sizes_two_ref[block], value * value, 0.0
                        )
                summed.append(
                    jnp.broadcast_to(jnp.sum(gathered, axis=1, keepdims=True), (CHUNK, LANES))
                )
            vectors_ref[pl.ds(12 + tile, 1), :] = jnp.sum(
                jnp.where(diag, jnp.concatenate(summed, axis=0), 0.0), axis=0, keepdims=True
            )

    slots, semaphores = plan_of_moves()
    work = items_of(slots)
    length = max(work) // 2 + 1
    looped = max(turn // 2 for turn in work if work[turn][0] == 0) + 1 + LOOPED
    slots = slots + [([], [])] * (length - len(slots))
    order = [work[turn][1] for turn in sorted(work) if work[turn][0] == 0]
    fetches = [order[:4]] + [[step] for step in order[4:]] + [[]] * length
    whole = [max(turn // 2 for turn in work if work[turn][0] == part) for part in range(PARTS)]
    extra = {5: [square_columns]}
    for part in range(PARTS - 1):
        for after, run in zip(AFTER[part], (first_onward, first_end)):
            extra.setdefault(min(whole[part] + after, length), []).append(
                functools.partial(run, part)
            )
    for total in totals:
        total[...] = jnp.zeros_like(total)
    moves(*slots[0], fetches[0])
    for copy in load_two:
        copy.start()
    total_one = jnp.float32(0)
    for block in range(sizes_one_ref.shape[0]):
        total_one = total_one + sizes_one_ref[block].astype(jnp.float32)
    total_two = jnp.float32(0)
    for block in range(sizes_two_ref.shape[0]):
        total_two = total_two + sizes_two_ref[block].astype(jnp.float32)
    all_one = jnp.full((TILES, LANES), total_one, jnp.float32)
    all_two = jnp.full((TILES, LANES), total_two, jnp.float32)
    log_one = jnp.log2(all_one)
    log_two = jnp.log2(all_two)
    def one_slot(slot, carry):
        for group in range(0, looped, 8):

            @pl.when((slot >= group) & (slot < group + 8))
            def _():
                for index in range(max(group, 1), min(group + 8, looped)):
                    if slots[index] != ([], []) or fetches[index] or index in extra:

                        @pl.when(slot == index)
                        def _():
                            moves(*slots[index], fetches[index])
                            for run in extra.get(index, ()):
                                run()

        def one_turn(turn, carry):
            code = jnp.int32(-1)
            for index, (part, step) in work.items():
                if index >= 2 * looped:
                    continue
                code = jnp.where(2 * slot + turn == index, part * len(STEPS) + step, code)

            @pl.when(code >= 0)
            def _():
                multiply(code)

            return carry

        lax.fori_loop(0, 2, one_turn, 0)
        for part in range(PARTS - 1):

            @pl.when(slot == whole[part])
            def _():
                first_start(part)

        return carry

    lax.fori_loop(0, looped, one_slot, 0)
    for index in range(looped, length):
        moves(*slots[index], fetches[index])
        for run in extra.get(index, ()):
            run()
        for turn in (2 * index, 2 * index + 1):
            if turn in work:
                step = work[turn][1]
                multiply_slim(step, [place(half, *STEPS[step]) - core for half in range(2)])
    first_start(PARTS - 1)
    for run in extra.get(length, ()):
        run()
    for tile in range(TILES):
        column = jnp.broadcast_to(
            jnp.sum(squares_ref[pl.ds(tile * LANES, LANES), :], axis=1, keepdims=True),
            (LANES, LANES),
        )
        vectors_ref[pl.ds(8 + tile, 1), :] = jnp.sum(
            jnp.where(diag, column, 0.0), axis=0, keepdims=True
        )
    first_onward(PARTS - 1)
    first_end(PARTS - 1)

    scale = jnp.float32(2.0 / math.sqrt(mass_scale) * math.log2(math.e))
    for start in range(0, BLOCK, CHUNK):
        rows = pl.ds(start, CHUNK)
        cost_ref[rows, :] = jnp.where(
            live_part(start, BLOCK), cost_ref[rows, :] * scale, jnp.float32(very_low)
        )

    def exchange(box, mine, sweep, send, recv, targets):
        for target in targets:
            pltpu.make_async_remote_copy(
                src_ref=box.at[sweep, mine],
                dst_ref=box.at[sweep, mine],
                send_sem=send.at[0],
                recv_sem=recv.at[sweep],
                device_id=target,
                device_id_type=MESH,
            ).start()
        wait_bytes(box.at[sweep, pl.ds(0, len(targets))], recv.at[sweep])
        logs = box[sweep]
        top = jnp.max(logs, axis=0)
        return top + jnp.log2(jnp.sum(jnp.exp2(logs - top[None]), axis=0))

    def gamma_row(gamma):
        return jnp.concatenate([gamma[t : t + 1, :] for t in range(TILES)], axis=1)

    def sweep_body(sweep, gamma):
        lines = []
        for tile in range(TILES):
            column = []
            for start in range(tile * LANES, (tile + 1) * LANES, CHUNK):
                values = cost_ref[pl.ds(start, CHUNK), :] + gamma_row(gamma)
                top = jnp.max(values, axis=1, keepdims=True)
                summed = jnp.sum(jnp.exp2(values - top), axis=1, keepdims=True)
                column.append(jnp.broadcast_to(top + jnp.log2(summed), (CHUNK, LANES)))
            column = jnp.concatenate(column, axis=0)
            lines.append(jnp.sum(jnp.where(diag, column, 0.0), axis=0, keepdims=True))
        row_box[sweep, col] = jnp.concatenate(lines, axis=0)
        lse = exchange(
            row_box, col, sweep, row_send, row_recv, [(row, peer) for peer in row_peers]
        )
        rho = jnp.where(live_row, -log_one - lse, 0.0)
        vectors_ref[pl.ds(0, TILES), :] = rho
        columns = []
        for tile in range(TILES):
            spread = jnp.broadcast_to(rho[tile : tile + 1, :], (LANES, LANES))
            columns.append(
                jnp.sum(jnp.where(diag, spread, 0.0), axis=1, keepdims=True)
            )
        for tile in range(TILES):
            rho_ref[pl.ds(tile * LANES, LANES), :] = jnp.broadcast_to(
                columns[tile], (LANES, LANES)
            )
        lines = []
        for tile in range(TILES):
            lanes = pl.ds(tile * LANES, LANES)
            tops, sums = [], []
            for start in range(0, BLOCK, 2 * CHUNK):
                rows = pl.ds(start, 2 * CHUNK)
                values = (cost_ref[rows, lanes] + rho_ref[rows, :]).reshape(
                    2 * CHUNK // 8, 8, LANES
                )
                top = jnp.max(values, axis=0)
                tops.append(top)
                sums.append(jnp.sum(jnp.exp2(values - top[None]), axis=0))
            high = functools.reduce(jnp.maximum, tops)
            high = jnp.max(high, axis=0, keepdims=True)
            summed = sum(s * jnp.exp2(t - high) for s, t in zip(sums, tops))
            lines.append(high + jnp.log2(jnp.sum(summed, axis=0, keepdims=True)))
        col_box[sweep, row] = jnp.concatenate(lines, axis=0)
        lse = exchange(
            col_box, row, sweep, col_send, col_recv, [(peer, col) for peer in col_peers]
        )
        return jnp.where(live_col, -log_two - lse, 0.0)

    gamma = lax.fori_loop(0, SWEEPS, sweep_body, jnp.zeros((TILES, LANES), jnp.float32))

    unit = jnp.float32(math.log(2.0) / math.sqrt(mass_scale))
    rho = vectors_ref[pl.ds(0, TILES), :]
    row_const = vectors_ref[pl.ds(8, TILES), :] / all_one
    col_const = vectors_ref[pl.ds(12, TILES), :] / all_two
    vectors_ref[pl.ds(4, TILES), :] = gamma
    vectors_ref[pl.ds(8, TILES), :] = jnp.where(live_row, rho * unit + row_const, 0.0)
    vectors_ref[pl.ds(12, TILES), :] = jnp.where(live_col, gamma * unit + col_const, 0.0)

    wait_bytes(row_box.at[:, pl.ds(0, 3)], row_send.at[0])
    wait_bytes(col_box.at[:, pl.ds(0, 31)], col_send.at[0])
    for part in range(PARTS):
        wait_bytes(plans[part].at[pl.ds(0, 31)], plan_send.at[part])
        wait_bytes(firsts[part].at[pl.ds(0, 3)], first_send.at[part])


def finish_kernel(
    mass_scale, cost_ref, rho_ref, vectors_ref, plan_ref, row_ref, col_ref, made_ref, made_sem
):
    gamma = jnp.concatenate([vectors_ref[pl.ds(4 + t, 1), :] for t in range(TILES)], axis=1)
    copies = []
    for start in range(0, BLOCK, LANES):
        rows = pl.ds(start, LANES)
        exponent = (
            cost_ref[rows, :] + jnp.concatenate([rho_ref[rows, :]] * TILES, axis=1) + gamma
        )
        made_ref[rows, :] = jnp.float32(mass_scale) * jnp.exp2(exponent)
        copy = pltpu.make_async_copy(
            made_ref.at[rows, :], plan_ref.at[rows, :], made_sem.at[start // LANES]
        )
        copy.start()
        copies.append(copy)
    row_ref[...] = vectors_ref[pl.ds(8, TILES), :]
    col_ref[...] = vectors_ref[pl.ds(12, TILES), :]
    for copy in copies:
        copy.wait()


def body(graph_one, graph_two, coupling, sizes_one, sizes_two):
    graph_one, graph_two, coupling, sizes_one, sizes_two = (
        pltpu.with_memory_space_constraint(value, pltpu.HBM)
        for value in (graph_one, graph_two, coupling, sizes_one, sizes_two)
    )
    mass_scale = float(graph_one.shape[1] * graph_two.shape[1])
    vmem = pl.BlockSpec(memory_space=pltpu.VMEM)
    smem = pl.BlockSpec(memory_space=pltpu.SMEM)
    hbm = pl.BlockSpec(memory_space=pltpu.HBM)
    f32, bf16 = jnp.float32, jnp.bfloat16
    dma = pltpu.SemaphoreType.DMA
    cost, rho, vectors = pl.pallas_call(
        functools.partial(gw_kernel, mass_scale),
        out_shape=(
            jax.ShapeDtypeStruct((BLOCK, BLOCK), f32),
            jax.ShapeDtypeStruct((BLOCK, LANES), f32),
            jax.ShapeDtypeStruct((4 * TILES, LANES), f32),
        ),
        in_specs=[hbm, hbm, hbm, smem, smem],
        out_specs=(vmem, vmem, vmem),
        scratch_shapes=[
            pltpu.VMEM((32, BLOCK, WIDTHS[0]), bf16),
            pltpu.VMEM((32, BLOCK, WIDTHS[1]), bf16),
            pltpu.VMEM((4, BLOCK, WIDTHS[0]), bf16),
            pltpu.VMEM((4, BLOCK, WIDTHS[1]), bf16),
            pltpu.VMEM((BLOCK, WIDTHS[0]), f32),
            pltpu.VMEM((BLOCK, WIDTHS[1]), f32),
            pltpu.VMEM((32, BLOCK, BLOCK), bf16),
            pltpu.VMEM((4, BLOCK, BLOCK), bf16),
            pltpu.VMEM((BLOCK, BLOCK), f32),
            pltpu.VMEM((BLOCK, LANES), f32),
            pltpu.VMEM((SWEEPS, 4, TILES, LANES), f32),
            pltpu.VMEM((SWEEPS, 32, TILES, LANES), f32),
            dma((2,)),
            dma((len(STEPS),)),
            dma((PARTS,)),
            dma((len(plan_of_moves()[1]),)),
            dma((PARTS, len(STEPS))),
            dma((PARTS,)),
            dma((PARTS, 4 + 2 * max(CUTS))),
            dma((1,)),
            dma((SWEEPS,)),
            dma((1,)),
            dma((SWEEPS,)),
        ],
        compiler_params=pltpu.CompilerParams(
            collective_id=0, has_side_effects=True, vmem_limit_bytes=52000 * 1024
        ),
        name="gw_step",
    )(graph_one, graph_two, coupling, sizes_one, sizes_two)
    plan, row_potential, col_potential = pl.pallas_call(
        functools.partial(finish_kernel, mass_scale),
        out_shape=(
            jax.ShapeDtypeStruct((BLOCK, BLOCK), f32),
            jax.ShapeDtypeStruct((TILES, LANES), f32),
            jax.ShapeDtypeStruct((TILES, LANES), f32),
        ),
        in_specs=[vmem, vmem, vmem],
        out_specs=(hbm, vmem, vmem),
        scratch_shapes=[pltpu.VMEM((BLOCK, BLOCK), f32), dma((TILES,))],
        compiler_params=pltpu.CompilerParams(vmem_limit_bytes=8 * 1024 * 1024),
        name="finish",
    )(cost, rho, vectors)
    return plan, row_potential.reshape(BLOCK), col_potential.reshape(BLOCK)


def solution(mesh):
    return jax.shard_map(
        body,
        mesh=mesh,
        in_specs=(P("row", None), P("col", None), P("row", "col"), P(), P()),
        out_specs=(P("row", "col"), P("row"), P("col")),
        check_vma=False,
    )
```
